128 devices in a mesh: gx: 16 (over x, y), gy: 4 (over z_hi, core), gz: 2 (over z_lo).
Axes of the slice: x: 4, y: 4, z: 4 (z_hi: 2, z_lo: 2; z = z_hi * 2 + z_lo), core: 2. Of those that a mesh axis runs over, the one named last changes fastest.
Arguments:
- right_side: float32 [256, 256, 1024], P('gx', 'gy', 'gz'), may hold values from -24 to 24
- reaction: float32 [256, 256, 1024], P('gx', 'gy', 'gz'), may hold values from 0.5 to 2
- velocity: float32 [3, 256, 256, 1024], P(None, 'gx', 'gy', 'gz'), may hold values from -0.5 to 0.5
Outputs:
- solution: float32 [256, 256, 1024], P('gx', 'gy', 'gz')
- residual: float32 [256, 256, 1024], P('gx', 'gy', 'gz')
- residual_norm: float32 [], replicated
The draws below stay inside these ranges and needn't reach their ends.
All inputs are finite; a program needn't handle non-finite values.
Results may differ from the reference program's by a relative error of at most 0.00002.
Values sent between devices are 32-bit elements; how exact they have to be, the bound alone decides.
No kernel may reach another device: no remote copies, remote signals or barrier semaphores. Data moves between devices by JAX's collectives and lax.ppermute only.
A program may use at most 128 MiB of HBM per device.

```python
import math
import jax
import jax.numpy as jnp

ITERS = 5
NX = 256
NY = 256
NZ = 1024


def draw_right_side(key, part):
    noise_key = jax.random.fold_in(jax.random.fold_in(key, 11), 0)
    ramp = 1.0 + 2.0 * jnp.arange(NX, dtype=jnp.float32)[:, None, None] / max(NX - 1, 1)
    values = ramp * jnp.clip(jax.random.normal(noise_key, (NX, NY, NZ), jnp.float32), -6.0, 6.0)
    return values.astype(jnp.float32)


def block_levels(own_key, extent, shards, least, top_value):
    def one(position, blocks):
        steps = jax.random.uniform(jax.random.fold_in(jax.random.fold_in(own_key, 6), position), (blocks,), jnp.float32, least / len(shards), top_value / len(shards))
        return jnp.repeat(jnp.exp(steps), extent[position] // blocks).reshape((-1,) + (1,) * (len(extent) - position - 1))

    loudness = one(*shards[0])
    for cut in shards[1:]:
        loudness = loudness * one(*cut)
    return loudness


def setup_inputs(seed: int = 0) -> dict:
    arg_keys = jax.random.split(jax.random.key(seed), 4)
    return {
        "right_side": draw_right_side(jax.random.fold_in(arg_keys[3], 71), 0),
        "reaction": jnp.clip(jnp.exp(math.log(2.0) - 1.3862944 * jax.random.uniform(arg_keys[1], (NX, NY, NZ), jnp.float32) ** block_levels(arg_keys[1], (NX, NY, NZ), ((0, 16), (1, 4), (2, 2)), -0.2, 0.2)), 0.5, 2.0),
        "velocity": jnp.clip(jax.random.uniform(arg_keys[2], (3, NX, NY, NZ), jnp.float32, -0.5, 0.5) * block_levels(arg_keys[2], (3, NX, NY, NZ), ((1, 16), (2, 4), (3, 2)), -0.4, 0.0), -0.5, 0.5),
    }


centre = 7.25
half_width = 6.75

def chebyshev_weights(count):
    ratio_value = centre / half_width
    weights = [1.0 / ratio_value]
    for iteration in range(count):
        weights.append(1.0 / (2.0 * ratio_value - weights[-1]))
    return weights

def combine(middle, plus_x, minus_x, plus_y, minus_y, plus_z, minus_z, reaction, velocity):
    beside = (1.0 - velocity[0]) * plus_x + (1.0 + velocity[0]) * minus_x
    beside = beside + (1.0 - velocity[1]) * plus_y + (1.0 + velocity[1]) * minus_y
    beside = beside + (1.0 - velocity[2]) * plus_z + (1.0 + velocity[2]) * minus_z
    return (6.0 + reaction) * middle - beside

def operate(values, reaction, velocity):
    plus_x = jnp.roll(values, -1, 0)
    minus_x = jnp.roll(values, 1, 0)
    padded = jnp.pad(values, ((0, 0), (1, 1), (1, 1)))
    return combine(values, plus_x, minus_x, padded[:, 2:, 1:-1], padded[:, :-2, 1:-1], padded[:, 1:-1, 2:], padded[:, 1:-1, :-2], reaction, velocity)

def reference(right_side, reaction, velocity):
    weights = chebyshev_weights(ITERS)
    solution = jnp.zeros_like(right_side)
    residual = right_side
    direction = right_side / centre
    for iteration in range(ITERS):
        applied = operate(direction, reaction, velocity)
        solution = solution + direction
        residual = residual - applied
        if iteration + 1 < ITERS:
            direction = weights[iteration + 1] * weights[iteration] * direction + 2.0 * weights[iteration + 1] / half_width * residual
    residual_norm = jnp.sqrt(jnp.sum(residual * residual) / (NX * NY * NZ) + 1e-06)
    return (solution, residual, residual_norm)
```

```python
import jax
import jax.numpy as jnp
from jax import lax
from jax.experimental import pallas as pl
from jax.experimental.pallas import tpu as pltpu
from jax.sharding import PartitionSpec as P

ITERS = 5
LANES = 128

centre = 7.25
half_width = 6.75


def chebyshev_weights(count):
    ratio_value = centre / half_width
    weights = [1.0 / ratio_value]
    for iteration in range(count):
        weights.append(1.0 / (2.0 * ratio_value - weights[-1]))
    return weights


def step_factors(iteration):
    weights = chebyshev_weights(ITERS)
    return weights[iteration + 1] * weights[iteration], 2.0 * weights[iteration + 1] / half_width


def in_vmem(shape):
    return pltpu.VMEM(shape, jnp.float32)


def call(body, name, out_shape, args, spaces, out_spaces, aliases=None, scratch=(), flops=0):
    spec = {
        "v": pl.BlockSpec(memory_space=pltpu.VMEM),
        "s": pl.BlockSpec(memory_space=pltpu.SMEM),
        "h": pl.BlockSpec(memory_space=pl.ANY),
    }
    args = [
        pltpu.with_memory_space_constraint(arg, pltpu.VMEM) if space == "v" else arg
        for arg, space in zip(args, spaces)
    ]
    return pl.pallas_call(
        body,
        name=name,
        out_shape=out_shape,
        in_specs=[spec[space] for space in spaces],
        out_specs=[spec[space] for space in out_spaces],
        input_output_aliases=aliases or {},
        scratch_shapes=list(scratch),
        compiler_params=pltpu.CompilerParams(vmem_limit_bytes=8 * 1024 * 1024),
        cost_estimate=pl.CostEstimate(flops=flops, bytes_accessed=0, transcendentals=0),
    )(*args)


def tile_iota(dim):
    return lax.broadcasted_iota(jnp.int32, (8, LANES), dim)


def column_tile(place_ref):
    high = place_ref[2] == 0
    offset = pl.multiple_of(jnp.where(high, 512 - LANES, 0), LANES)
    return offset, jnp.where(high, LANES - 1, 0)


def pack_columns(read, offset, lane, out_ref, scale=None):
    lanes = tile_iota(1)
    for t in range(8):
        packed = jnp.zeros((8, LANES), jnp.float32)
        for i in range(16):
            tile = read(i, t, offset)
            moved = pltpu.roll(tile, lax.rem(i - lane + LANES, LANES), 1)
            packed = jnp.where(lanes == i, moved, packed)
        if scale is not None:
            packed = packed * scale
        out_ref[8 * t : 8 * t + 8, :] = packed


def write_faces(read_plane, d_ref, place_ref, xlo, xhi, ylo, yhi, zface, scale=None):
    def scaled(value):
        return value if scale is None else value * scale

    xlo[...] = scaled(d_ref[0])
    xhi[...] = scaled(d_ref[15])
    for i in range(16):
        ylo[i : i + 1, :] = scaled(d_ref[i, 0:1, :])
        yhi[i : i + 1, :] = scaled(d_ref[i, 63:64, :])
    offset, lane = column_tile(place_ref)
    pack_columns(
        lambda i, t, off: d_ref[i, 8 * t : 8 * t + 8, pl.ds(off, LANES)], offset, lane, zface, scale
    )


FACES = [(64, 512), (64, 512), (16, 512), (16, 512), (64, LANES)]


def first_faces(place_ref, rhs_ref, *faces):
    write_faces(None, rhs_ref, place_ref, *faces, scale=1.0 / centre)


def neighbours(d_ref, i, t, row, scale=None):
    def load(plane, tile):
        value = d_ref[plane, 8 * tile : 8 * tile + 8, :]
        return value if scale is None else value * scale

    here = load(i, t)
    above = load(i, (t + 1) % 8)
    below = load(i, (t + 7) % 8)
    plus_x = load(lax.rem(i + 1, 16), t)
    minus_x = load(lax.rem(i + 15, 16), t)
    plus_y = pltpu.roll(jnp.where(row == 0, above, here), 7, 0)
    minus_y = pltpu.roll(jnp.where(row == 7, below, here), 1, 0)
    plus_z = pltpu.roll(here, 511, 1)
    minus_z = pltpu.roll(here, 1, 1)
    return here, plus_x, minus_x, plus_y, minus_y, plus_z, minus_z


def first_main(place_ref, rhs_ref, reaction_ref, velocity_ref, diag_ref, up_ref, down_ref, r_ref, d_ref, d0_ref,
               xlo_c, xhi_c, ylo_c, yhi_c, z_c):
    factor, gain = step_factors(0)
    row = lax.broadcasted_iota(jnp.int32, (8, 512), 0)
    col = lax.broadcasted_iota(jnp.int32, (8, 512), 1)
    has_below = (place_ref[0] > 0).astype(jnp.float32)
    has_above = (place_ref[1] > 0).astype(jnp.float32)

    def plane(i, carry):
        first = jnp.where(i == 0, 0.0, 1.0)
        last = jnp.where(i == 15, 0.0, 1.0)
        for t in range(8):
            rows = slice(8 * t, 8 * t + 8)
            here, px, mx, py, my, pz, mz = neighbours(rhs_ref, i, t, row, 1.0 / centre)
            vx = velocity_ref[0, i, rows, :]
            vy = velocity_ref[1, i, rows, :]
            vz = velocity_ref[2, i, rows, :]
            diag = 6.0 + reaction_ref[i, rows, :]
            up_x = (1.0 - vx) * last
            down_x = (1.0 + vx) * first
            up_y = 1.0 - vy
            down_y = 1.0 + vy
            if t == 0:
                ylo_c[i] = jnp.where(row == 0, down_y * has_below, 0.0)
                down_y = jnp.where(row == 0, 0.0, down_y)
            if t == 7:
                yhi_c[i] = jnp.where(row == 7, up_y * has_above, 0.0)
                up_y = jnp.where(row == 7, 0.0, up_y)
            up_z = jnp.where(col == 511, 0.0, 1.0 - vz)
            down_z = jnp.where(col == 0, 0.0, 1.0 + vz)
            diag_ref[i, rows, :] = diag
            up_ref[0, i, rows, :] = up_x
            up_ref[1, i, rows, :] = up_y
            up_ref[2, i, rows, :] = up_z
            down_ref[0, i, rows, :] = down_x
            down_ref[1, i, rows, :] = down_y
            down_ref[2, i, rows, :] = down_z
            beside = up_x * px + down_x * mx + (up_y * py + down_y * my) + (up_z * pz + down_z * mz)
            residual = rhs_ref[i, rows, :] - (diag * here - beside)
            r_ref[i, rows, :] = residual
            d0_ref[i, rows, :] = here
            d_ref[i, rows, :] = factor * here + gain * residual
        return carry

    lax.fori_loop(0, 16, plane, 0)
    xlo_c[...] = 1.0 + velocity_ref[0, 0]
    xhi_c[...] = 1.0 - velocity_ref[0, 15]
    offset, lane = column_tile(place_ref)
    sign = jnp.where(place_ref[2] == 0, -1.0, 1.0)
    pack_columns(
        lambda i, t, off: 1.0 + sign * velocity_ref[2, i, 8 * t : 8 * t + 8, pl.ds(off, LANES)], offset, lane, z_c
    )


def main(factor, gain, d_ref, r_ref, s_ref, diag_ref, up_ref, down_ref, r_out, d_out, s_out):
    row = lax.broadcasted_iota(jnp.int32, (8, 512), 0)

    def plane(i, carry):
        for t in range(8):
            rows = slice(8 * t, 8 * t + 8)
            here, px, mx, py, my, pz, mz = neighbours(d_ref, i, t, row)
            beside = up_ref[0, i, rows, :] * px + down_ref[0, i, rows, :] * mx
            beside = beside + (up_ref[1, i, rows, :] * py + down_ref[1, i, rows, :] * my)
            beside = beside + (up_ref[2, i, rows, :] * pz + down_ref[2, i, rows, :] * mz)
            residual = r_ref[i, rows, :] - (diag_ref[i, rows, :] * here - beside)
            r_out[i, rows, :] = residual
            s_out[i, rows, :] = s_ref[i, rows, :] + here
            d_out[i, rows, :] = factor * here + gain * residual
        return carry

    lax.fori_loop(0, 16, plane, 0)


def last_main(d_ref, r_ref, s_ref, diag_ref, up_ref, down_ref, r_out, s_out, s_buf, sem):
    row = lax.broadcasted_iota(jnp.int32, (8, 512), 0)

    def plane(i, carry):
        for t in range(8):
            rows = slice(8 * t, 8 * t + 8)
            here, px, mx, py, my, pz, mz = neighbours(d_ref, i, t, row)
            beside = up_ref[0, i, rows, :] * px + down_ref[0, i, rows, :] * mx
            beside = beside + (up_ref[1, i, rows, :] * py + down_ref[1, i, rows, :] * my)
            beside = beside + (up_ref[2, i, rows, :] * pz + down_ref[2, i, rows, :] * mz)
            r_out[i, rows, :] = r_ref[i, rows, :] - (diag_ref[i, rows, :] * here - beside)
            s_buf[i, rows, :] = s_ref[i, rows, :] + here
        return carry

    lax.fori_loop(0, 16, plane, 0)
    copy = pltpu.make_async_copy(s_buf, s_out, sem)
    copy.start()
    copy.wait()


def correct(gain, place_ref, halos, coefs, r_ref, d_ref):
    hxm, hxp, hym, hyp, hz = halos
    xlo_c, xhi_c, ylo_c, yhi_c, z_c = coefs

    def add(i, rows, lanes, change):
        r_ref[i, rows, lanes] = r_ref[i, rows, lanes] + change
        if d_ref is not None:
            d_ref[i, rows, lanes] = d_ref[i, rows, lanes] + gain * change

    every = slice(None)
    add(0, every, every, xlo_c[...] * hxm[...])
    add(15, every, every, xhi_c[...] * hxp[...])
    for i in range(16):
        add(i, slice(0, 8), every, ylo_c[i] * jnp.broadcast_to(hym[i : i + 1, :], (8, 512)))
        add(i, slice(56, 64), every, yhi_c[i] * jnp.broadcast_to(hyp[i : i + 1, :], (8, 512)))
    offset, lane = column_tile(place_ref)
    lanes = tile_iota(1)
    for t in range(8):
        rows = slice(8 * t, 8 * t + 8)
        change = z_c[rows, :] * hz[rows, :]
        for i in range(16):
            moved = pltpu.roll(change, lax.rem(lane - i + LANES, LANES), 1)
            add(i, rows, pl.ds(offset, LANES), jnp.where(lanes == lane, moved, 0.0))


def fix(gain, place_ref, *refs):
    halos, coefs, (_, _), (r_ref, d_ref), faces = refs[:5], refs[5:10], refs[10:12], refs[12:14], refs[14:]
    correct(gain, place_ref, halos, coefs, r_ref, d_ref)
    write_faces(None, d_ref, place_ref, *faces)


def last_fix(place_ref, *refs):
    halos, coefs = refs[:5], refs[5:10]
    _, r_ref, r_hbm, part_ref, sem = refs[10:]
    correct(None, place_ref, halos, coefs, r_ref, None)
    copy = pltpu.make_async_copy(r_ref, r_hbm, sem)
    copy.start()

    def plane(i, total):
        for t in range(8):
            value = r_ref[i, 8 * t : 8 * t + 8, :]
            total = total + value * value
        return total

    total = lax.fori_loop(0, 16, plane, jnp.zeros((8, 512), jnp.float32))
    part_ref[...] = jnp.broadcast_to(jnp.sum(total).reshape(1, 1), part_ref.shape)
    copy.wait()


def finish(cells, got_ref, out_ref):
    total = jnp.sum(got_ref[...], axis=0, keepdims=True)
    out_ref[...] = jnp.sqrt(total / cells + 1e-06)


def local(right_side, reaction, velocity):
    gx, gy = lax.axis_size("gx"), lax.axis_size("gy")
    me_y, me_z = lax.axis_index("gy"), lax.axis_index("gz")
    place = jnp.stack([(me_y > 0).astype(jnp.int32), (me_y < gy - 1).astype(jnp.int32), me_z.astype(jnp.int32)])
    shape = right_side.shape
    block = in_vmem(shape)
    face_shapes = [in_vmem(face) for face in FACES]

    def exchange(faces):
        xlo, xhi, ylo, yhi, zface = faces
        up = lambda n: [(i, (i + 1) % n) for i in range(n)]
        down = lambda n: [((i + 1) % n, i) for i in range(n)]
        return [
            lax.ppermute(xhi, "gx", up(gx)),
            lax.ppermute(xlo, "gx", down(gx)),
            lax.ppermute(yhi, "gy", up(gy)),
            lax.ppermute(ylo, "gy", down(gy)),
            lax.ppermute(zface, "gz", up(2)),
        ]

    faces = call(first_faces, "first_faces", face_shapes, [place, right_side], "sv", "vvvvv")
    halos = exchange(faces)
    diag, up, down, r, d, d0, *coefs = call(
        first_main,
        "first_main",
        [block, in_vmem((3,) + shape), in_vmem((3,) + shape), block, block, block]
        + [in_vmem(s) for s in [(64, 512), (64, 512), (16, 8, 512), (16, 8, 512), (64, LANES)]],
        [place, right_side, reaction, velocity],
        "svvv",
        "v" * 11,
        flops=10**8,
    )
    s = d0
    for iteration in range(ITERS):
        if iteration > 0:
            halos = exchange(faces)
            if iteration + 1 < ITERS:
                factor, gain = step_factors(iteration)
                r, d, s = call(
                    lambda *refs, factor=factor, gain=gain: main(factor, gain, *refs),
                    "main",
                    [block] * 3,
                    [d, r, s, diag, up, down],
                    "vvvvvv",
                    "vvv",
                    flops=10**8,
                )
            else:
                r, solution_out = call(
                    last_main,
                    "last_main",
                    [block, jax.ShapeDtypeStruct(shape, jnp.float32)],
                    [d, r, s, diag, up, down],
                    "vvvvvv",
                    "vh",
                    scratch=[pltpu.VMEM(shape, jnp.float32), pltpu.SemaphoreType.DMA],
                    flops=10**8,
                )
        if iteration + 1 < ITERS:
            gain = step_factors(iteration)[1]
            r, d, *faces = call(
                lambda *refs, gain=gain: fix(gain, *refs),
                "fix",
                [block, block] + face_shapes,
                [place, *halos, *coefs, r, d],
                "s" + "v" * 12,
                "v" * 7,
                aliases={11: 0, 12: 1},
            )
    devices = gx * gy * lax.axis_size("gz")
    _, residual, part = call(
        last_fix,
        "last_fix",
        [block, jax.ShapeDtypeStruct(shape, jnp.float32), in_vmem((devices, LANES))],
        [place, *halos, *coefs, r],
        "s" + "v" * 11,
        "vhv",
        aliases={11: 0},
        scratch=[pltpu.SemaphoreType.DMA],
    )
    part = part.reshape(devices, 1, LANES)
    got = lax.all_to_all(part, ("gx", "gy", "gz"), 0, 0, tiled=True).reshape(devices, LANES)
    cells = shape[0] * shape[1] * shape[2] * devices
    norm = call(
        lambda *refs: finish(cells, *refs), "finish", [in_vmem((1, LANES))], [got], "v", "v"
    )[0]
    return solution_out, residual, norm[0, 0]


def solution(mesh):
    return jax.shard_map(
        local,
        mesh=mesh,
        in_specs=(P("gx", "gy", "gz"), P("gx", "gy", "gz"), P(None, "gx", "gy", "gz")),
        out_specs=(P("gx", "gy", "gz"), P("gx", "gy", "gz"), P()),
        check_vma=False,
    )
```

```python
import functools

import jax
import jax.numpy as jnp
from jax import lax
from jax.experimental import pallas as pl
from jax.experimental.pallas import tpu as pltpu
from jax.sharding import PartitionSpec as P

ITERS = 5
LANES = 128

centre = 7.25
half_width = 6.75


def chebyshev_weights(count):
    ratio_value = centre / half_width
    weights = [1.0 / ratio_value]
    for iteration in range(count):
        weights.append(1.0 / (2.0 * ratio_value - weights[-1]))
    return weights


def step_factors(iteration):
    weights = chebyshev_weights(ITERS)
    return weights[iteration + 1] * weights[iteration], 2.0 * weights[iteration + 1] / half_width


def in_vmem(shape):
    return pltpu.VMEM(shape, jnp.float32)


def call(body, name, out_shape, args, spaces, out_spaces, aliases=None, scratch=(), flops=0, limit=4):
    spec = {
        "v": pl.BlockSpec(memory_space=pltpu.VMEM),
        "s": pl.BlockSpec(memory_space=pltpu.SMEM),
        "h": pl.BlockSpec(memory_space=pl.ANY),
    }
    args = [
        arg if space == "s" else pltpu.with_memory_space_constraint(arg, pltpu.VMEM if space == "v" else pltpu.HBM)
        for arg, space in zip(args, spaces)
    ]
    return pl.pallas_call(
        body,
        name=name,
        out_shape=out_shape,
        in_specs=[spec[space] for space in spaces],
        out_specs=[spec[space] for space in out_spaces],
        input_output_aliases=aliases or {},
        scratch_shapes=list(scratch),
        compiler_params=pltpu.CompilerParams(vmem_limit_bytes=limit * 1024 * 1024),
        cost_estimate=pl.CostEstimate(flops=flops, bytes_accessed=0, transcendentals=0),
    )(*args)


def tile_iota(dim):
    return lax.broadcasted_iota(jnp.int32, (8, LANES), dim)


def column_tile(place_ref):
    high = place_ref[3] == 0
    offset = pl.multiple_of(jnp.where(high, 512 - LANES, 0), LANES)
    return offset, jnp.where(high, LANES - 1, 0)


def pack_columns(read, offset, lane, out_ref, scale=None):
    lanes = tile_iota(1)
    for t in range(8):
        packed = jnp.zeros((8, LANES), jnp.float32)
        for i in range(16):
            tile = read(i, t, offset)
            moved = pltpu.roll(tile, lax.rem(i - lane + LANES, LANES), 1)
            packed = jnp.where(lanes == i, moved, packed)
        if scale is not None:
            packed = packed * scale
        out_ref[8 * t : 8 * t + 8, :] = packed


def sides(place_ref):
    even_x = place_ref[0] == 0
    even_y = place_ref[1] == 0
    planes = jnp.where(even_x, 15, 0), jnp.where(even_x, 0, 15)
    rows = jnp.where(even_y, 63, 0), jnp.where(even_y, 0, 63)
    tiles = [pl.multiple_of(jnp.where(even_y, high, low), 8) for high, low in ((56, 0), (0, 56))]
    return planes, rows, tiles


def write_faces(d_ref, place_ref, xa, xb, ya, yb, zface, scale=None):
    def scaled(value):
        return value if scale is None else value * scale

    planes, rows, _ = sides(place_ref)
    xa[...] = scaled(d_ref[planes[0]])
    xb[...] = scaled(d_ref[planes[1]])
    for face, row in ((ya, rows[0]), (yb, rows[1])):
        values = [d_ref[i, pl.ds(row, 1), :] for i in range(16)]
        for i in range(16):
            face[i : i + 1, :] = scaled(values[i])
    offset, lane = column_tile(place_ref)
    pack_columns(
        lambda i, t, off: d_ref[i, 8 * t : 8 * t + 8, pl.ds(off, LANES)], offset, lane, zface, scale
    )


FACES = [(64, 512), (64, 512), (16, 512), (16, 512), (64, LANES)]


def first_faces(place_ref, rhs_ref, *faces):
    write_faces(rhs_ref, place_ref, *faces, scale=1.0 / centre)


def row_of_tiles(ref, i, t):
    return [ref[i, 8 * t : 8 * t + 8, LANES * j : LANES * j + LANES] for j in range(4)]


def plane_terms(values_ref, reaction_ref, velocity_ref, i, has_plus, has_minus, emit):
    row, lane = tile_iota(0), tile_iota(1)
    zero = jnp.zeros((8, LANES), jnp.float32)
    below = [zero] * 4
    here = row_of_tiles(values_ref, i, 0)
    for t in range(8):
        rows = slice(8 * t, 8 * t + 8)
        above = row_of_tiles(values_ref, i, t + 1) if t < 7 else [zero] * 4
        left = [pltpu.roll(tile, 1, 1) for tile in here]
        right = [pltpu.roll(tile, LANES - 1, 1) for tile in here]
        for j in range(4):
            lanes = slice(LANES * j, LANES * j + LANES)
            plus_y = pltpu.roll(jnp.where(row == 0, above[j], here[j]), 7, 0)
            minus_y = pltpu.roll(jnp.where(row == 7, below[j], here[j]), 1, 0)
            plus_z = jnp.where(lane == LANES - 1, right[j + 1] if j < 3 else zero, right[j])
            minus_z = jnp.where(lane == 0, left[j - 1] if j > 0 else zero, left[j])
            beside = (plus_y + minus_y) + (plus_z + minus_z)
            skew = velocity_ref[1, i, rows, lanes] * (plus_y - minus_y)
            skew = skew + velocity_ref[2, i, rows, lanes] * (plus_z - minus_z)
            vx = velocity_ref[0, i, rows, lanes]
            if has_plus and has_minus:
                plus_x = values_ref[i + 1, rows, lanes]
                minus_x = values_ref[i - 1, rows, lanes]
                beside = beside + (plus_x + minus_x)
                skew = skew + vx * (plus_x - minus_x)
            elif has_plus:
                plus_x = values_ref[i + 1, rows, lanes]
                beside = beside + plus_x
                skew = skew + vx * plus_x
            else:
                minus_x = values_ref[i - 1, rows, lanes]
                beside = beside + minus_x
                skew = skew - vx * minus_x
            applied = (6.0 + reaction_ref[i, rows, lanes]) * here[j] - (beside - skew)
            emit(i, rows, lanes, here[j], applied)
        below, here = here, above


def over_planes(body):
    body(0, True, False)

    def inner(i, carry):
        body(i, True, True)
        return carry

    lax.fori_loop(1, 15, inner, 0)
    body(15, False, True)


def first_main(place_ref, rhs_ref, reaction_hbm, velocity_hbm, reaction_ref, velocity_ref, r_ref, d_ref,
               xa_c, xb_c, ya_c, yb_c, z_c, sems):
    factor, gain = step_factors(0)

    def copies(i):
        return (
            pltpu.make_async_copy(reaction_hbm.at[i], reaction_ref.at[i], sems.at[0, i]),
            pltpu.make_async_copy(velocity_hbm.at[:, i], velocity_ref.at[:, i], sems.at[1, i]),
        )

    for i in range(16):
        for copy in copies(i):
            copy.start()

    def emit(i, rows, lanes, here, applied):
        residual = here - applied * (1.0 / centre)
        r_ref[i, rows, lanes] = residual
        d_ref[i, rows, lanes] = (factor / centre) * here + gain * residual

    def body(i, has_plus, has_minus):
        for copy in copies(i):
            copy.wait()
        plane_terms(rhs_ref, reaction_ref, velocity_ref, i, has_plus, has_minus, emit)

    over_planes(body)
    planes, _, tiles = sides(place_ref)
    sign_x = jnp.where(place_ref[0] == 0, -1.0, 1.0)
    sign_y = jnp.where(place_ref[1] == 0, -1.0, 1.0)
    inside = (place_ref[2] > 0).astype(jnp.float32)
    row = lax.broadcasted_iota(jnp.int32, (8, 512), 0)
    xa_c[...] = 1.0 + sign_x * velocity_ref[0, planes[0]]
    xb_c[...] = 1.0 - sign_x * velocity_ref[0, planes[1]]
    row_a = jnp.where(place_ref[1] == 0, 7, 0)
    for i in range(16):
        own_a = 1.0 + sign_y * velocity_ref[1, i, pl.ds(tiles[0], 8), :]
        own_b = (1.0 - sign_y * velocity_ref[1, i, pl.ds(tiles[1], 8), :]) * inside
        ya_c[i] = jnp.where(row == row_a, own_a, 0.0)
        yb_c[i] = jnp.where(row == 7 - row_a, own_b, 0.0)
    offset, lane = column_tile(place_ref)
    sign = jnp.where(place_ref[3] == 0, -1.0, 1.0)
    pack_columns(
        lambda i, t, off: 1.0 + sign * velocity_ref[2, i, 8 * t : 8 * t + 8, pl.ds(off, LANES)], offset, lane, z_c
    )


def main(factor, gain, s_scale, d_ref, r_ref, s_ref, reaction_ref, velocity_ref, r_out, d_out, s_out):
    def emit(i, rows, lanes, here, applied):
        residual = r_ref[i, rows, lanes] - applied
        r_out[i, rows, lanes] = residual
        before = s_ref[i, rows, lanes]
        s_out[i, rows, lanes] = (before if s_scale is None else before * s_scale) + here
        d_out[i, rows, lanes] = factor * here + gain * residual

    over_planes(lambda i, plus, minus: plane_terms(d_ref, reaction_ref, velocity_ref, i, plus, minus, emit))


def last_main(d_ref, r_ref, s_ref, reaction_ref, velocity_ref, r_out, s_out, s_buf, sem):
    def emit(i, rows, lanes, here, applied):
        r_out[i, rows, lanes] = r_ref[i, rows, lanes] - applied
        s_buf[i, rows, lanes] = s_ref[i, rows, lanes] + here

    def body(i, plus, minus):
        plane_terms(d_ref, reaction_ref, velocity_ref, i, plus, minus, emit)
        pltpu.make_async_copy(s_buf.at[i], s_out.at[i], sem.at[i]).start()

    over_planes(body)
    for i in range(16):
        pltpu.make_async_copy(s_buf.at[i], s_out.at[i], sem.at[i]).wait()


def correct(gain, place_ref, halos, coefs, r_ref, d_ref):
    hxa, hxb, hya, hyb, hz = halos
    xa_c, xb_c, ya_c, yb_c, z_c = coefs
    planes, _, tiles = sides(place_ref)

    def add(places, changes):
        new_r = [r_ref[at] + change for at, change in zip(places, changes)]
        if d_ref is not None:
            new_d = [d_ref[at] + gain * change for at, change in zip(places, changes)]
        for n, at in enumerate(places):
            r_ref[at] = new_r[n]
            if d_ref is not None:
                d_ref[at] = new_d[n]

    for t in range(0, 64, 16):
        rows = slice(t, t + 16)
        add([(planes[0], rows)], [xa_c[rows, :] * hxa[rows, :]])
        add([(planes[1], rows)], [xb_c[rows, :] * hxb[rows, :]])
    for first in range(0, 16, 4):
        group = range(first, first + 4)
        for tile, coef, halo in ((tiles[0], ya_c, hya), (tiles[1], yb_c, hyb)):
            changes = [coef[i] * jnp.broadcast_to(halo[i : i + 1, :], (8, 512)) for i in group]
            add([(i, pl.ds(tile, 8)) for i in group], changes)
    offset, lane = column_tile(place_ref)
    lanes = tile_iota(1)
    shifts = [lax.rem(lane - i + LANES, LANES) for i in range(16)]
    for t in range(8):
        rows = slice(8 * t, 8 * t + 8)
        change = z_c[rows, :] * hz[rows, :]
        moved = [jnp.where(lanes == lane, pltpu.roll(change, shift, 1), 0.0) for shift in shifts]
        add([(i, rows, pl.ds(offset, LANES)) for i in range(16)], moved)


def fix(gain, place_ref, *refs):
    halos, coefs, (_, _), (r_ref, d_ref), faces = refs[:5], refs[5:10], refs[10:12], refs[12:14], refs[14:]
    correct(gain, place_ref, halos, coefs, r_ref, d_ref)
    write_faces(d_ref, place_ref, *faces)


def last_fix(place_ref, *refs):
    halos, coefs = refs[:5], refs[5:10]
    _, r_ref, r_hbm, part_ref, sem = refs[10:]
    correct(None, place_ref, halos, coefs, r_ref, None)
    copy = pltpu.make_async_copy(r_ref, r_hbm, sem)
    copy.start()

    def plane(i, total):
        for t in range(8):
            value = r_ref[i, 8 * t : 8 * t + 8, :]
            total = total + value * value
        return total

    total = lax.fori_loop(0, 16, plane, jnp.zeros((8, 512), jnp.float32))
    part_ref[...] = jnp.broadcast_to(jnp.sum(total).reshape(1, 1), part_ref.shape)
    copy.wait()


def finish(cells, got_ref, out_ref):
    total = jnp.sum(got_ref[...], axis=0, keepdims=True)
    out_ref[...] = jnp.sqrt(total / cells + 1e-06)


def local(right_side, reaction, velocity):
    gx, gy, gz = lax.axis_size("gx"), lax.axis_size("gy"), lax.axis_size("gz")
    me_x, me_y, me_z = lax.axis_index("gx"), lax.axis_index("gy"), lax.axis_index("gz")
    inside = ((me_y > 0) & (me_y < gy - 1)).astype(jnp.int32)
    place = jnp.stack([me_x % 2, me_y % 2, inside, me_z]).astype(jnp.int32)
    shape = right_side.shape
    block = in_vmem(shape)
    face_shapes = [in_vmem(face) for face in FACES]

    def pairs(n, first):
        step = [1 - 2 * (i % 2) if first else 2 * (i % 2) - 1 for i in range(n)]
        return [(i, (i + step[i]) % n) for i in range(n)]

    def exchange(faces):
        xa, xb, ya, yb, zface = faces
        return [
            lax.ppermute(xa, "gx", pairs(gx, True)),
            lax.ppermute(xb, "gx", pairs(gx, False)),
            lax.ppermute(ya, "gy", pairs(gy, True)),
            lax.ppermute(yb, "gy", pairs(gy, False)),
            lax.ppermute(zface, "gz", pairs(gz, True)),
        ]

    faces = call(first_faces, "first_faces", face_shapes, [place, right_side], "sv", "vvvvv")
    halos = exchange(faces)
    reaction_v, velocity_v, r, d, *coefs = call(
        first_main,
        "first_main",
        [block, in_vmem((3,) + shape), block, block]
        + [in_vmem(s) for s in [(64, 512), (64, 512), (16, 8, 512), (16, 8, 512), (64, LANES)]],
        [place, right_side, reaction, velocity],
        "svhh",
        "v" * 9,
        scratch=[pltpu.SemaphoreType.DMA((2, 16))],
        flops=10**8,
    )
    s = right_side
    for iteration in range(ITERS):
        if iteration > 0:
            halos = exchange(faces)
            if iteration + 1 < ITERS:
                factor, gain = step_factors(iteration)
                r, d, s = call(
                    functools.partial(main, factor, gain, 1.0 / centre if iteration == 1 else None),
                    "main",
                    [block] * 3,
                    [d, r, s, reaction_v, velocity_v],
                    "vvvvv",
                    "vvv",
                    flops=10**8,
                )
            else:
                r, solution_out = call(
                    last_main,
                    "last_main",
                    [block, pltpu.HBM(shape, jnp.float32)],
                    [d, r, s, reaction_v, velocity_v],
                    "vvvvv",
                    "vh",
                    scratch=[pltpu.VMEM(shape, jnp.float32), pltpu.SemaphoreType.DMA((16,))],
                    flops=10**8,
                )
        if iteration + 1 < ITERS:
            gain = step_factors(iteration)[1]
            r, d, *faces = call(
                functools.partial(fix, gain),
                "fix",
                [block, block] + face_shapes,
                [place, *halos, *coefs, r, d],
                "s" + "v" * 12,
                "v" * 7,
                aliases={11: 0, 12: 1},
            )
    devices = gx * gy * gz
    _, residual, part = call(
        last_fix,
        "last_fix",
        [block, pltpu.HBM(shape, jnp.float32), in_vmem((devices, LANES))],
        [place, *halos, *coefs, r],
        "s" + "v" * 11,
        "vhv",
        aliases={11: 0},
        scratch=[pltpu.SemaphoreType.DMA],
    )
    part = part.reshape(devices, 1, LANES)
    got = lax.all_to_all(part, ("gx", "gy", "gz"), 0, 0, tiled=True).reshape(devices, LANES)
    cells = shape[0] * shape[1] * shape[2] * devices
    norm = call(
        functools.partial(finish, cells), "finish", [in_vmem((1, LANES))], [got], "v", "v"
    )[0]
    return solution_out, residual, norm[0, 0]


def solution(mesh):
    return jax.shard_map(
        local,
        mesh=mesh,
        in_specs=(P("gx", "gy", "gz"), P("gx", "gy", "gz"), P(None, "gx", "gy", "gz")),
        out_specs=(P("gx", "gy", "gz"), P("gx", "gy", "gz"), P()),
        check_vma=False,
    )
```

```python
import functools

import jax
import jax.numpy as jnp
from jax import lax
from jax.experimental import pallas as pl
from jax.experimental.pallas import tpu as pltpu
from jax.sharding import PartitionSpec as P

ITERS = 5
LANES = 128
COST = 10**8

centre = 7.25
half_width = 6.75


def chebyshev_weights(count):
    ratio_value = centre / half_width
    weights = [1.0 / ratio_value]
    for iteration in range(count):
        weights.append(1.0 / (2.0 * ratio_value - weights[-1]))
    return weights


def step_factors(iteration):
    weights = chebyshev_weights(ITERS)
    return weights[iteration + 1] * weights[iteration], 2.0 * weights[iteration + 1] / half_width


def in_vmem(shape):
    return pltpu.VMEM(shape, jnp.float32)


def call(body, name, out_shape, args, spaces, out_spaces, aliases=None, scratch=(), flops=0, limit=4, nbytes=0):
    spec = {
        "v": pl.BlockSpec(memory_space=pltpu.VMEM),
        "s": pl.BlockSpec(memory_space=pltpu.SMEM),
        "h": pl.BlockSpec(memory_space=pl.ANY),
    }
    args = [
        arg if space == "s" else pltpu.with_memory_space_constraint(arg, pltpu.VMEM if space == "v" else pltpu.HBM)
        for arg, space in zip(args, spaces)
    ]
    return pl.pallas_call(
        body,
        name=name,
        out_shape=out_shape,
        in_specs=[spec[space] for space in spaces],
        out_specs=[spec[space] for space in out_spaces],
        input_output_aliases=aliases or {},
        scratch_shapes=list(scratch),
        compiler_params=pltpu.CompilerParams(vmem_limit_bytes=limit * 1024 * 1024),
        cost_estimate=pl.CostEstimate(flops=flops, bytes_accessed=nbytes, transcendentals=0),
    )(*args)


def position():
    me_y, last_y = lax.axis_index("gy"), lax.axis_size("gy") - 1
    inside = jnp.where((me_y > 0) & (me_y < last_y), 1, 0)
    return lax.rem(lax.axis_index("gx"), 2), lax.rem(me_y, 2), inside, lax.axis_index("gz")


def tile_iota(dim):
    return lax.broadcasted_iota(jnp.int32, (8, LANES), dim)


def column_tile(place):
    high = place[3] == 0
    offset = pl.multiple_of(jnp.where(high, 512 - LANES, 0), LANES)
    return offset, jnp.where(high, LANES - 1, 0)


def pack_columns(read, offset, lane, out_ref, scale=None):
    lanes = tile_iota(1)
    for t in range(8):
        packed = jnp.zeros((8, LANES), jnp.float32)
        for i in range(16):
            tile = read(i, t, offset)
            moved = pltpu.roll(tile, lax.rem(i - lane + LANES, LANES), 1)
            packed = jnp.where(lanes == i, moved, packed)
        if scale is not None:
            packed = packed * scale
        out_ref[8 * t : 8 * t + 8, :] = packed


def sides(place):
    even_x = place[0] == 0
    even_y = place[1] == 0
    planes = jnp.where(even_x, 15, 0), jnp.where(even_x, 0, 15)
    rows = jnp.where(even_y, 63, 0), jnp.where(even_y, 0, 63)
    tiles = [pl.multiple_of(jnp.where(even_y, high, low), 8) for high, low in ((56, 0), (0, 56))]
    return planes, rows, tiles


def write_side_faces(rows_at, tile_at, place, ya, yb, zface):
    for n, face in enumerate((ya, yb)):
        values = [rows_at(n, i) for i in range(16)]
        for i in range(16):
            face[i : i + 1, :] = values[i]
    offset, lane = column_tile(place)
    pack_columns(lambda i, t, off: tile_at(i, t), offset, lane, zface)


FACES = [(64, 512), (64, 512), (16, 512), (16, 512), (64, LANES)]


def first_x_faces(rhs_hbm, xa, xb, sem):
    planes, _, _ = sides(position())
    copies = [pltpu.make_async_copy(rhs_hbm.at[plane], face, sem.at[n])
              for n, (plane, face) in enumerate(zip(planes, (xa, xb)))]
    for copy in copies:
        copy.start()
    for copy in copies:
        copy.wait()


def first_side_faces(rhs_hbm, ya, yb, zface, rows_a, rows_b, column, sem):
    place = position()
    _, rows, tiles = sides(place)
    offset, _ = column_tile(place)
    copies = [
        pltpu.make_async_copy(rhs_hbm.at[:, pl.ds(tiles[0], 8), :], rows_a, sem.at[0]),
        pltpu.make_async_copy(rhs_hbm.at[:, pl.ds(tiles[1], 8), :], rows_b, sem.at[1]),
        pltpu.make_async_copy(rhs_hbm.at[:, :, pl.ds(offset, LANES)], column, sem.at[2]),
    ]
    for copy in copies:
        copy.start()
    for copy in copies:
        copy.wait()
    held = rows_a, rows_b
    write_side_faces(
        lambda n, i: held[n][i, pl.ds(lax.rem(rows[n], 8), 1), :],
        lambda i, t: column[i, 8 * t : 8 * t + 8, :],
        place, ya, yb, zface,
    )


def row_of_tiles(ref, i, t):
    return [ref[i, 8 * t : 8 * t + 8, LANES * j : LANES * j + LANES] for j in range(4)]


def plane_terms(values_ref, diagonal, velocity_ref, i, has_plus, has_minus, emit):
    row, lane = tile_iota(0), tile_iota(1)
    zero = jnp.zeros((8, LANES), jnp.float32)
    below = [zero] * 4
    here = row_of_tiles(values_ref, i, 0)
    for t in range(8):
        rows = slice(8 * t, 8 * t + 8)
        above = row_of_tiles(values_ref, i, t + 1) if t < 7 else [zero] * 4
        left = [pltpu.roll(tile, 1, 1) for tile in here]
        right = [pltpu.roll(tile, LANES - 1, 1) for tile in here]
        for j in range(4):
            lanes = slice(LANES * j, LANES * j + LANES)
            plus_y = pltpu.roll(jnp.where(row == 0, above[j], here[j]), 7, 0)
            minus_y = pltpu.roll(jnp.where(row == 7, below[j], here[j]), 1, 0)
            plus_z = jnp.where(lane == LANES - 1, right[j + 1] if j < 3 else zero, right[j])
            minus_z = jnp.where(lane == 0, left[j - 1] if j > 0 else zero, left[j])
            beside = (plus_y + minus_y) + (plus_z + minus_z)
            skew = velocity_ref[1, i, rows, lanes] * (plus_y - minus_y)
            skew = skew + velocity_ref[2, i, rows, lanes] * (plus_z - minus_z)
            vx = velocity_ref[0, i, rows, lanes]
            if has_plus and has_minus:
                plus_x = values_ref[i + 1, rows, lanes]
                minus_x = values_ref[i - 1, rows, lanes]
                beside = beside + (plus_x + minus_x)
                skew = skew + vx * (plus_x - minus_x)
            elif has_plus:
                plus_x = values_ref[i + 1, rows, lanes]
                beside = beside + plus_x
                skew = skew + vx * plus_x
            else:
                minus_x = values_ref[i - 1, rows, lanes]
                beside = beside + minus_x
                skew = skew - vx * minus_x
            applied = diagonal(i, rows, lanes) * here[j] - (beside - skew)
            emit(i, rows, lanes, here[j], applied)
        below, here = here, above


def over_planes(body):
    body(0, True, False)

    def inner(i, carry):
        body(i, True, True)
        return carry

    lax.fori_loop(1, 15, inner, 0, unroll=2)
    body(15, False, True)


def first_main(rhs_ref, reaction_ref, velocity_ref, r_ref, d_ref, diag_ref, xa_c, xb_c, ya_c, yb_c, z_c):
    place = position()
    factor, gain = step_factors(0)

    def diagonal(i, rows, lanes):
        value = 6.0 + reaction_ref[i, rows, lanes]
        diag_ref[i, rows, lanes] = value
        return value

    def emit(i, rows, lanes, here, applied):
        residual = here - applied * (1.0 / centre)
        r_ref[i, rows, lanes] = residual
        d_ref[i, rows, lanes] = (factor / centre) * here + gain * residual

    over_planes(lambda i, plus, minus: plane_terms(rhs_ref, diagonal, velocity_ref, i, plus, minus, emit))
    planes, _, tiles = sides(place)
    sign_x = jnp.where(place[0] == 0, -1.0, 1.0)
    sign_y = jnp.where(place[1] == 0, -1.0, 1.0)
    inside = (place[2] > 0).astype(jnp.float32)
    row = lax.broadcasted_iota(jnp.int32, (8, 512), 0)
    xa_c[...] = 1.0 + sign_x * velocity_ref[0, planes[0]]
    xb_c[...] = 1.0 - sign_x * velocity_ref[0, planes[1]]
    row_a = jnp.where(place[1] == 0, 7, 0)
    for i in range(16):
        own_a = 1.0 + sign_y * velocity_ref[1, i, pl.ds(tiles[0], 8), :]
        own_b = (1.0 - sign_y * velocity_ref[1, i, pl.ds(tiles[1], 8), :]) * inside
        ya_c[i] = jnp.where(row == row_a, own_a, 0.0)
        yb_c[i] = jnp.where(row == 7 - row_a, own_b, 0.0)
    offset, lane = column_tile(place)
    sign = jnp.where(place[3] == 0, -1.0, 1.0)
    pack_columns(
        lambda i, t, off: 1.0 + sign * velocity_ref[2, i, 8 * t : 8 * t + 8, pl.ds(off, LANES)], offset, lane, z_c
    )


def held(ref):
    return lambda i, rows, lanes: ref[i, rows, lanes]


def main(factor, gain, s_scale, d_ref, r_ref, s_ref, diag_ref, velocity_ref, r_out, d_out, s_out):
    def emit(i, rows, lanes, here, applied):
        residual = r_ref[i, rows, lanes] - applied
        r_out[i, rows, lanes] = residual
        before = s_ref[i, rows, lanes]
        s_out[i, rows, lanes] = (before if s_scale is None else before * s_scale) + here
        d_out[i, rows, lanes] = factor * here + gain * residual

    over_planes(lambda i, plus, minus: plane_terms(d_ref, held(diag_ref), velocity_ref, i, plus, minus, emit))


def last_main(d_ref, r_ref, s_ref, diag_ref, velocity_ref, r_out, s_out, s_buf, sem):
    def emit(i, rows, lanes, here, applied):
        r_out[i, rows, lanes] = r_ref[i, rows, lanes] - applied
        s_buf[i, rows, lanes] = s_ref[i, rows, lanes] + here

    def body(i, plus, minus):
        plane_terms(d_ref, held(diag_ref), velocity_ref, i, plus, minus, emit)
        pltpu.make_async_copy(s_buf.at[i], s_out.at[i], sem.at[i]).start()

    over_planes(body)
    for i in range(16):
        pltpu.make_async_copy(s_buf.at[i], s_out.at[i], sem.at[i]).wait()


def correct(gain, place, scale, halos, coefs, r_ref, d_ref, ends, inner):
    hxa, hxb, hya, hyb, hz = halos
    xa_c, xb_c, ya_c, yb_c, z_c = coefs
    planes, _, tiles = sides(place)
    which = ([0, 15] if ends else []) + (list(range(1, 15)) if inner else [])

    def term(coef, halo):
        return coef * halo if scale is None else coef * halo * scale

    def add(places, changes):
        new_r = [r_ref[at] + change for at, change in zip(places, changes)]
        if d_ref is not None:
            new_d = [d_ref[at] + gain * change for at, change in zip(places, changes)]
        for n, at in enumerate(places):
            r_ref[at] = new_r[n]
            if d_ref is not None:
                d_ref[at] = new_d[n]

    if ends:
        for t in range(0, 64, 16):
            rows = slice(t, t + 16)
            add([(planes[0], rows)], [term(xa_c[rows, :], hxa[rows, :])])
            add([(planes[1], rows)], [term(xb_c[rows, :], hxb[rows, :])])
    for first in range(0, len(which), 4):
        group = which[first : first + 4]
        for tile, coef, halo in ((tiles[0], ya_c, hya), (tiles[1], yb_c, hyb)):
            changes = [term(coef[i], jnp.broadcast_to(halo[i : i + 1, :], (8, 512))) for i in group]
            add([(i, pl.ds(tile, 8)) for i in group], changes)
    offset, lane = column_tile(place)
    lanes = tile_iota(1)
    shifts = {i: lax.rem(lane - i + LANES, LANES) for i in which}
    for t in range(8):
        rows = slice(8 * t, 8 * t + 8)
        change = term(z_c[rows, :], hz[rows, :])
        moved = [jnp.where(lanes == lane, pltpu.roll(change, shifts[i], 1), 0.0) for i in which]
        add([(i, rows, pl.ds(offset, LANES)) for i in which], moved)


def fix_ends(gain, scale, *refs):
    halos, coefs, (_, _), (r_ref, d_ref, xa, xb) = refs[:5], refs[5:10], refs[10:12], refs[12:]
    place = position()
    correct(gain, place, scale, halos, coefs, r_ref, d_ref, True, False)
    planes, _, _ = sides(place)
    xa[...] = d_ref[planes[0]]
    xb[...] = d_ref[planes[1]]


def fix_inner(gain, scale, *refs):
    (hya, hyb, hz), (ya_c, yb_c, z_c), (_, _), (r_ref, d_ref, ya, yb, zface) = refs[:3], refs[3:6], refs[6:8], refs[8:]
    place = position()
    halos, coefs = (None, None, hya, hyb, hz), (None, None, ya_c, yb_c, z_c)
    correct(gain, place, scale, halos, coefs, r_ref, d_ref, False, True)
    _, rows, _ = sides(place)
    offset, _ = column_tile(place)
    write_side_faces(
        lambda n, i: d_ref[i, pl.ds(rows[n], 1), :],
        lambda i, t: d_ref[i, 8 * t : 8 * t + 8, pl.ds(offset, LANES)],
        place, ya, yb, zface,
    )


def last_fix(*refs):
    halos, coefs = refs[:5], refs[5:10]
    _, r_ref, part_ref = refs[10:]
    correct(None, position(), None, halos, coefs, r_ref, None, True, True)

    def plane(i, total):
        for t in range(8):
            value = r_ref[i, 8 * t : 8 * t + 8, :]
            total = total + value * value
        return total

    total = lax.fori_loop(0, 16, plane, jnp.zeros((8, 512), jnp.float32), unroll=2)
    part_ref[...] = jnp.broadcast_to(jnp.sum(total).reshape(1, 1), part_ref.shape)


def finish(cells, got_ref, out_ref):
    total = jnp.sum(got_ref[...], axis=0, keepdims=True)
    out_ref[...] = jnp.sqrt(total / cells + 1e-06)


def local(right_side, reaction, velocity):
    gx, gy, gz = lax.axis_size("gx"), lax.axis_size("gy"), lax.axis_size("gz")
    shape = right_side.shape
    block = in_vmem(shape)
    face_shapes = [in_vmem(face) for face in FACES]

    def pairs(n, first):
        step = [1 - 2 * (i % 2) if first else 2 * (i % 2) - 1 for i in range(n)]
        return [(i, (i + step[i]) % n) for i in range(n)]

    def exchange_x(xa, xb):
        far = lax.ppermute(xb, "gx", pairs(gx, False))
        return [lax.ppermute(xa, "gx", pairs(gx, True)), far]

    def exchange_sides(ya, yb, zface):
        return [
            lax.ppermute(ya, "gy", pairs(gy, True)),
            lax.ppermute(yb, "gy", pairs(gy, False)),
            lax.ppermute(zface, "gz", pairs(gz, True)),
        ]

    halos = exchange_x(
        *call(first_x_faces, "first_x_faces", face_shapes[:2], [right_side], "h", "vv",
              scratch=[pltpu.SemaphoreType.DMA((2,))], flops=COST)
    )
    rows = pltpu.VMEM((16, 8, 512), jnp.float32)
    halos += exchange_sides(
        *call(first_side_faces, "first_side_faces", face_shapes[2:], [right_side], "h", "vvv",
              scratch=[rows, rows, pltpu.VMEM((16, 64, LANES), jnp.float32), pltpu.SemaphoreType.DMA((3,))], flops=COST)
    )
    r, d, diag, *coefs = call(
        first_main,
        "first_main",
        [block, block, block]
        + [in_vmem(s) for s in [(64, 512), (64, 512), (16, 8, 512), (16, 8, 512), (64, LANES)]],
        [right_side, reaction, velocity],
        "vvv",
        "v" * 8,
        flops=COST,
    )
    s = right_side
    for iteration in range(ITERS):
        if iteration > 0:
            if iteration + 1 < ITERS:
                factor, gain = step_factors(iteration)
                r, d, s = call(
                    functools.partial(main, factor, gain, 1.0 / centre if iteration == 1 else None),
                    "main",
                    [block] * 3,
                    [d, r, s, diag, velocity],
                    "vvvvv",
                    "vvv",
                    flops=COST,
                )
            else:
                r, solution_out = call(
                    last_main,
                    "last_main",
                    [block, pltpu.HBM(shape, jnp.float32)],
                    [d, r, s, diag, velocity],
                    "vvvvv",
                    "vh",
                    scratch=[pltpu.VMEM(shape, jnp.float32), pltpu.SemaphoreType.DMA((16,))],
                    flops=COST,
                )
        if iteration + 1 < ITERS:
            gain = step_factors(iteration)[1]
            scale = 1.0 / centre if iteration == 0 else None
            r, d, *x_faces = call(
                functools.partial(fix_ends, gain, scale),
                "fix_ends",
                [block, block] + face_shapes[:2],
                [*halos, *coefs, r, d],
                "v" * 12,
                "v" * 4,
                aliases={10: 0, 11: 1},
            )
            next_halos = exchange_x(*x_faces)
            r, d, *side_faces = call(
                functools.partial(fix_inner, gain, scale),
                "fix_inner",
                [block, block] + face_shapes[2:],
                [*halos[2:], *coefs[2:], r, d],
                "v" * 8,
                "v" * 5,
                aliases={6: 0, 7: 1},
            )
            halos = next_halos + exchange_sides(*side_faces)
    devices = gx * gy * gz
    residual, part = call(
        last_fix,
        "last_fix",
        [block, in_vmem((devices, LANES))],
        [*halos, *coefs, r],
        "v" * 11,
        "vv",
        aliases={10: 0},
    )
    part = part.reshape(devices, 1, LANES)
    got = lax.all_to_all(part, ("gx", "gy", "gz"), 0, 0, tiled=True).reshape(devices, LANES)
    cells = shape[0] * shape[1] * shape[2] * devices
    norm = call(
        functools.partial(finish, cells), "finish", [in_vmem((1, LANES))], [got], "v", "v"
    )[0]
    return solution_out, residual, norm[0, 0]


def solution(mesh):
    return jax.shard_map(
        local,
        mesh=mesh,
        in_specs=(P("gx", "gy", "gz"), P("gx", "gy", "gz"), P(None, "gx", "gy", "gz")),
        out_specs=(P("gx", "gy", "gz"), P("gx", "gy", "gz"), P()),
        check_vma=False,
    )
```

```python
import functools

import jax
import jax.numpy as jnp
from jax import lax
from jax.experimental import pallas as pl
from jax.experimental.pallas import tpu as pltpu
from jax.sharding import PartitionSpec as P

ITERS = 5
LANES = 128
COST = 10**8

centre = 7.25
half_width = 6.75


def chebyshev_weights(count):
    ratio_value = centre / half_width
    weights = [1.0 / ratio_value]
    for iteration in range(count):
        weights.append(1.0 / (2.0 * ratio_value - weights[-1]))
    return weights


def step_factors(iteration):
    weights = chebyshev_weights(ITERS)
    return weights[iteration + 1] * weights[iteration], 2.0 * weights[iteration + 1] / half_width


def in_vmem(shape):
    return pltpu.VMEM(shape, jnp.float32)


def call(body, name, out_shape, args, spaces, out_spaces, aliases=None, scratch=(), flops=0, limit=4, nbytes=0):
    spec = {
        "v": pl.BlockSpec(memory_space=pltpu.VMEM),
        "s": pl.BlockSpec(memory_space=pltpu.SMEM),
        "h": pl.BlockSpec(memory_space=pl.ANY),
    }
    args = [
        arg if space == "s" else pltpu.with_memory_space_constraint(arg, pltpu.VMEM if space == "v" else pltpu.HBM)
        for arg, space in zip(args, spaces)
    ]
    return pl.pallas_call(
        body,
        name=name,
        out_shape=out_shape,
        in_specs=[spec[space] for space in spaces],
        out_specs=[spec[space] for space in out_spaces],
        input_output_aliases=aliases or {},
        scratch_shapes=list(scratch),
        compiler_params=pltpu.CompilerParams(vmem_limit_bytes=limit * 1024 * 1024),
        cost_estimate=pl.CostEstimate(flops=flops, bytes_accessed=nbytes, transcendentals=0),
    )(*args)


def position():
    me_y, last_y = lax.axis_index("gy"), lax.axis_size("gy") - 1
    inside = jnp.where((me_y > 0) & (me_y < last_y), 1, 0)
    return lax.rem(lax.axis_index("gx"), 2), lax.rem(me_y, 2), inside, lax.axis_index("gz")


def tile_iota(dim):
    return lax.broadcasted_iota(jnp.int32, (8, LANES), dim)


def column_tile(place):
    high = place[3] == 0
    offset = pl.multiple_of(jnp.where(high, 512 - LANES, 0), LANES)
    return offset, jnp.where(high, LANES - 1, 0)


def pack_columns(read, offset, lane, out_ref, scale=None):
    lanes = tile_iota(1)
    for t in range(8):
        packed = jnp.zeros((8, LANES), jnp.float32)
        for i in range(16):
            tile = read(i, t, offset)
            moved = pltpu.roll(tile, lax.rem(i - lane + LANES, LANES), 1)
            packed = jnp.where(lanes == i, moved, packed)
        if scale is not None:
            packed = packed * scale
        out_ref[8 * t : 8 * t + 8, :] = packed


def sides(place):
    even_x = place[0] == 0
    even_y = place[1] == 0
    planes = jnp.where(even_x, 15, 0), jnp.where(even_x, 0, 15)
    rows = jnp.where(even_y, 63, 0), jnp.where(even_y, 0, 63)
    tiles = [pl.multiple_of(jnp.where(even_y, high, low), 8) for high, low in ((56, 0), (0, 56))]
    return planes, rows, tiles


def write_side_faces(rows_at, tile_at, place, ya, yb, zface):
    for n, face in enumerate((ya, yb)):
        values = [rows_at(n, i) for i in range(16)]
        for i in range(16):
            face[i : i + 1, :] = values[i]
    offset, lane = column_tile(place)
    pack_columns(lambda i, t, off: tile_at(i, t), offset, lane, zface)


FACES = [(64, 512), (64, 512), (16, 512), (16, 512), (64, LANES)]


def first_faces(rhs_hbm, xa, xb, ya, yb, zface, rows_a, rows_b, column, sem):
    place = position()
    planes, rows, tiles = sides(place)
    offset, _ = column_tile(place)
    copies = [
        pltpu.make_async_copy(rhs_hbm.at[:, :, pl.ds(offset, LANES)], column, sem.at[0]),
        pltpu.make_async_copy(rhs_hbm.at[:, pl.ds(tiles[0], 8), :], rows_a, sem.at[1]),
        pltpu.make_async_copy(rhs_hbm.at[:, pl.ds(tiles[1], 8), :], rows_b, sem.at[2]),
        pltpu.make_async_copy(rhs_hbm.at[planes[0]], xa, sem.at[3]),
        pltpu.make_async_copy(rhs_hbm.at[planes[1]], xb, sem.at[4]),
    ]
    for copy in copies:
        copy.start()
    for copy in copies[:3]:
        copy.wait()
    held = rows_a, rows_b
    write_side_faces(
        lambda n, i: held[n][i, pl.ds(lax.rem(rows[n], 8), 1), :],
        lambda i, t: column[i, 8 * t : 8 * t + 8, :],
        place, ya, yb, zface,
    )
    for copy in copies[3:]:
        copy.wait()


def row_of_tiles(ref, i, t):
    return [ref[i, 8 * t : 8 * t + 8, LANES * j : LANES * j + LANES] for j in range(4)]


def plane_terms(values_ref, diagonal, velocity_ref, i, has_plus, has_minus, emit):
    row, lane = tile_iota(0), tile_iota(1)
    zero = jnp.zeros((8, LANES), jnp.float32)
    below = [zero] * 4
    here = row_of_tiles(values_ref, i, 0)
    for t in range(8):
        rows = slice(8 * t, 8 * t + 8)
        above = row_of_tiles(values_ref, i, t + 1) if t < 7 else [zero] * 4
        left = [pltpu.roll(tile, 1, 1) for tile in here]
        right = [pltpu.roll(tile, LANES - 1, 1) for tile in here]
        for j in range(4):
            lanes = slice(LANES * j, LANES * j + LANES)
            plus_y = pltpu.roll(jnp.where(row == 0, above[j], here[j]), 7, 0)
            minus_y = pltpu.roll(jnp.where(row == 7, below[j], here[j]), 1, 0)
            plus_z = jnp.where(lane == LANES - 1, right[j + 1] if j < 3 else zero, right[j])
            minus_z = jnp.where(lane == 0, left[j - 1] if j > 0 else zero, left[j])
            beside = (plus_y + minus_y) + (plus_z + minus_z)
            skew = velocity_ref[1, i, rows, lanes] * (plus_y - minus_y)
            skew = skew + velocity_ref[2, i, rows, lanes] * (plus_z - minus_z)
            vx = velocity_ref[0, i, rows, lanes]
            if has_plus and has_minus:
                plus_x = values_ref[i + 1, rows, lanes]
                minus_x = values_ref[i - 1, rows, lanes]
                beside = beside + (plus_x + minus_x)
                skew = skew + vx * (plus_x - minus_x)
            elif has_plus:
                plus_x = values_ref[i + 1, rows, lanes]
                beside = beside + plus_x
                skew = skew + vx * plus_x
            else:
                minus_x = values_ref[i - 1, rows, lanes]
                beside = beside + minus_x
                skew = skew - vx * minus_x
            applied = diagonal(i, rows, lanes) * here[j] - (beside - skew)
            emit(i, rows, lanes, here[j], applied)
        below, here = here, above


def over_planes(body):
    body(0, True, False)

    def inner(i, carry):
        body(i, True, True)
        return carry

    lax.fori_loop(1, 15, inner, 0, unroll=2)
    body(15, False, True)


def first_main(rhs_ref, reaction_ref, velocity_ref, r_ref, d_ref, diag_ref, xa_c, xb_c, ya_c, yb_c, z_c):
    place = position()
    factor, gain = step_factors(0)

    def diagonal(i, rows, lanes):
        value = 6.0 + reaction_ref[i, rows, lanes]
        diag_ref[i, rows, lanes] = value
        return value

    def emit(i, rows, lanes, here, applied):
        residual = here - applied * (1.0 / centre)
        r_ref[i, rows, lanes] = residual
        d_ref[i, rows, lanes] = (factor / centre) * here + gain * residual

    over_planes(lambda i, plus, minus: plane_terms(rhs_ref, diagonal, velocity_ref, i, plus, minus, emit))
    planes, _, tiles = sides(place)
    sign_x = jnp.where(place[0] == 0, -1.0, 1.0)
    sign_y = jnp.where(place[1] == 0, -1.0, 1.0)
    inside = (place[2] > 0).astype(jnp.float32)
    row = lax.broadcasted_iota(jnp.int32, (8, 512), 0)
    xa_c[...] = 1.0 + sign_x * velocity_ref[0, planes[0]]
    xb_c[...] = 1.0 - sign_x * velocity_ref[0, planes[1]]
    row_a = jnp.where(place[1] == 0, 7, 0)
    for i in range(16):
        own_a = 1.0 + sign_y * velocity_ref[1, i, pl.ds(tiles[0], 8), :]
        own_b = (1.0 - sign_y * velocity_ref[1, i, pl.ds(tiles[1], 8), :]) * inside
        ya_c[i] = jnp.where(row == row_a, own_a, 0.0)
        yb_c[i] = jnp.where(row == 7 - row_a, own_b, 0.0)
    offset, lane = column_tile(place)
    sign = jnp.where(place[3] == 0, -1.0, 1.0)
    pack_columns(
        lambda i, t, off: 1.0 + sign * velocity_ref[2, i, 8 * t : 8 * t + 8, pl.ds(off, LANES)], offset, lane, z_c
    )


def held(ref):
    return lambda i, rows, lanes: ref[i, rows, lanes]


def main(factor, gain, s_scale, d_ref, r_ref, s_ref, diag_ref, velocity_ref, r_out, d_out, s_out):
    def emit(i, rows, lanes, here, applied):
        residual = r_ref[i, rows, lanes] - applied
        r_out[i, rows, lanes] = residual
        before = s_ref[i, rows, lanes]
        s_out[i, rows, lanes] = (before if s_scale is None else before * s_scale) + here
        d_out[i, rows, lanes] = factor * here + gain * residual

    over_planes(lambda i, plus, minus: plane_terms(d_ref, held(diag_ref), velocity_ref, i, plus, minus, emit))


def last_main(d_ref, r_ref, s_ref, diag_ref, velocity_ref, r_out, s_out):
    def emit(i, rows, lanes, here, applied):
        r_out[i, rows, lanes] = r_ref[i, rows, lanes] - applied
        s_out[i, rows, lanes] = s_ref[i, rows, lanes] + here

    over_planes(lambda i, plus, minus: plane_terms(d_ref, held(diag_ref), velocity_ref, i, plus, minus, emit))


def correct(gain, place, scale, halos, coefs, r_ref, d_ref, ends, inner):
    hxa, hxb, hya, hyb, hz = halos
    xa_c, xb_c, ya_c, yb_c, z_c = coefs
    planes, _, tiles = sides(place)
    which = ([0, 15] if ends else []) + (list(range(1, 15)) if inner else [])

    def term(coef, halo):
        return coef * halo if scale is None else coef * halo * scale

    def add(places, changes):
        new_r = [r_ref[at] + change for at, change in zip(places, changes)]
        if d_ref is not None:
            new_d = [d_ref[at] + gain * change for at, change in zip(places, changes)]
        for n, at in enumerate(places):
            r_ref[at] = new_r[n]
            if d_ref is not None:
                d_ref[at] = new_d[n]

    if ends:
        for t in range(0, 64, 16):
            rows = slice(t, t + 16)
            add([(planes[0], rows)], [term(xa_c[rows, :], hxa[rows, :])])
            add([(planes[1], rows)], [term(xb_c[rows, :], hxb[rows, :])])
    for first in range(0, len(which), 4):
        group = which[first : first + 4]
        for tile, coef, halo in ((tiles[0], ya_c, hya), (tiles[1], yb_c, hyb)):
            changes = [term(coef[i], jnp.broadcast_to(halo[i : i + 1, :], (8, 512))) for i in group]
            add([(i, pl.ds(tile, 8)) for i in group], changes)
    offset, lane = column_tile(place)
    lanes = tile_iota(1)
    shifts = {i: lax.rem(lane - i + LANES, LANES) for i in which}
    for t in range(8):
        rows = slice(8 * t, 8 * t + 8)
        change = term(z_c[rows, :], hz[rows, :])
        moved = [jnp.where(lanes == lane, pltpu.roll(change, shifts[i], 1), 0.0) for i in which]
        add([(i, rows, pl.ds(offset, LANES)) for i in which], moved)


def fix_ends(gain, scale, *refs):
    halos, coefs, (_, _), (r_ref, d_ref, xa, xb) = refs[:5], refs[5:10], refs[10:12], refs[12:]
    place = position()
    correct(gain, place, scale, halos, coefs, r_ref, d_ref, True, False)
    planes, _, _ = sides(place)
    xa[...] = d_ref[planes[0]]
    xb[...] = d_ref[planes[1]]


def fix_inner(gain, scale, *refs):
    (hya, hyb, hz), (ya_c, yb_c, z_c), (_, _), (r_ref, d_ref, ya, yb, zface) = refs[:3], refs[3:6], refs[6:8], refs[8:]
    place = position()
    halos, coefs = (None, None, hya, hyb, hz), (None, None, ya_c, yb_c, z_c)
    correct(gain, place, scale, halos, coefs, r_ref, d_ref, False, True)
    _, rows, _ = sides(place)
    offset, _ = column_tile(place)
    write_side_faces(
        lambda n, i: d_ref[i, pl.ds(rows[n], 1), :],
        lambda i, t: d_ref[i, 8 * t : 8 * t + 8, pl.ds(offset, LANES)],
        place, ya, yb, zface,
    )


def last_fix(*refs):
    halos, coefs = refs[:5], refs[5:10]
    _, r_ref, part_ref = refs[10:]
    correct(None, position(), None, halos, coefs, r_ref, None, True, True)

    def plane(i, total):
        for t in range(8):
            value = r_ref[i, 8 * t : 8 * t + 8, :]
            total = total + value * value
        return total

    total = lax.fori_loop(0, 16, plane, jnp.zeros((8, 512), jnp.float32), unroll=2)
    part_ref[...] = jnp.broadcast_to(jnp.sum(total).reshape(1, 1), part_ref.shape)


def save(held_ref, out_hbm, sem):
    copy = pltpu.make_async_copy(held_ref, out_hbm, sem)
    copy.start()
    copy.wait()


def finish(cells, got_ref, out_ref):
    total = jnp.sum(got_ref[...], axis=0, keepdims=True)
    out_ref[...] = jnp.sqrt(total / cells + 1e-06)


def local(right_side, reaction, velocity):
    gx, gy, gz = lax.axis_size("gx"), lax.axis_size("gy"), lax.axis_size("gz")
    shape = right_side.shape
    block = in_vmem(shape)
    face_shapes = [in_vmem(face) for face in FACES]

    def pairs(n, first):
        step = [1 - 2 * (i % 2) if first else 2 * (i % 2) - 1 for i in range(n)]
        return [(i, (i + step[i]) % n) for i in range(n)]

    def exchange_x(xa, xb):
        far = lax.ppermute(xb, "gx", pairs(gx, False))
        return [lax.ppermute(xa, "gx", pairs(gx, True)), far]

    def exchange_sides(ya, yb, zface):
        return [
            lax.ppermute(ya, "gy", pairs(gy, True)),
            lax.ppermute(yb, "gy", pairs(gy, False)),
            lax.ppermute(zface, "gz", pairs(gz, True)),
        ]

    rows = pltpu.VMEM((16, 8, 512), jnp.float32)
    faces = call(
        first_faces,
        "first_faces",
        face_shapes,
        [right_side],
        "h",
        "vvvvv",
        scratch=[rows, rows, pltpu.VMEM((16, 64, LANES), jnp.float32), pltpu.SemaphoreType.DMA((5,))],
        flops=100 * COST,
    )
    halos = exchange_x(*faces[:2]) + exchange_sides(*faces[2:])
    r, d, diag, *coefs = call(
        first_main,
        "first_main",
        [block, block, block]
        + [in_vmem(s) for s in [(64, 512), (64, 512), (16, 8, 512), (16, 8, 512), (64, LANES)]],
        [right_side, reaction, velocity],
        "vvv",
        "v" * 8,
        flops=COST,
    )
    s = right_side
    for iteration in range(ITERS):
        if iteration > 0:
            if iteration + 1 < ITERS:
                factor, gain = step_factors(iteration)
                r, d, s = call(
                    functools.partial(main, factor, gain, 1.0 / centre if iteration == 1 else None),
                    "main",
                    [block] * 3,
                    [d, r, s, diag, velocity],
                    "vvvvv",
                    "vvv",
                    flops=COST,
                )
            else:
                r, s = call(
                    last_main, "last_main", [block, block], [d, r, s, diag, velocity], "vvvvv", "vv", flops=COST
                )
        if iteration + 1 < ITERS:
            gain = step_factors(iteration)[1]
            scale = 1.0 / centre if iteration == 0 else None
            r, d, *x_faces = call(
                functools.partial(fix_ends, gain, scale),
                "fix_ends",
                [block, block] + face_shapes[:2],
                [*halos, *coefs, r, d],
                "v" * 12,
                "v" * 4,
                aliases={10: 0, 11: 1},
            )
            next_halos = exchange_x(*x_faces)
            r, d, *side_faces = call(
                functools.partial(fix_inner, gain, scale),
                "fix_inner",
                [block, block] + face_shapes[2:],
                [*halos[2:], *coefs[2:], r, d],
                "v" * 8,
                "v" * 5,
                aliases={6: 0, 7: 1},
            )
            halos = next_halos + exchange_sides(*side_faces)
    devices = gx * gy * gz
    residual, part = call(
        last_fix,
        "last_fix",
        [block, in_vmem((devices, LANES))],
        [*halos, *coefs, r],
        "v" * 11,
        "vv",
        aliases={10: 0},
    )
    solution_out = call(
        save, "save", [pltpu.HBM(shape, jnp.float32)], [s], "v", "h", scratch=[pltpu.SemaphoreType.DMA], flops=COST
    )[0]
    part = part.reshape(devices, 1, LANES)
    got = lax.all_to_all(part, ("gx", "gy", "gz"), 0, 0, tiled=True).reshape(devices, LANES)
    cells = shape[0] * shape[1] * shape[2] * devices
    norm = call(
        functools.partial(finish, cells), "finish", [in_vmem((1, LANES))], [got], "v", "v"
    )[0]
    return solution_out, residual, norm[0, 0]


def solution(mesh):
    return jax.shard_map(
        local,
        mesh=mesh,
        in_specs=(P("gx", "gy", "gz"), P("gx", "gy", "gz"), P(None, "gx", "gy", "gz")),
        out_specs=(P("gx", "gy", "gz"), P("gx", "gy", "gz"), P()),
        check_vma=False,
    )
```

```python
import functools

import jax
import jax.numpy as jnp
from jax import lax
from jax.experimental import pallas as pl
from jax.experimental.pallas import tpu as pltpu
from jax.sharding import PartitionSpec as P


ITERS = 5
LANES = 128
COST = 10**8

centre = 7.25
half_width = 6.75


def chebyshev_weights(count):
    ratio_value = centre / half_width
    weights = [1.0 / ratio_value]
    for _ in range(count):
        weights.append(1.0 / (2.0 * ratio_value - weights[-1]))
    return weights


def step_factors(iteration):
    weights = chebyshev_weights(ITERS)
    return weights[iteration + 1] * weights[iteration], 2.0 * weights[iteration + 1] / half_width


def in_vmem(shape):
    return pltpu.VMEM(shape, jnp.float32)


def call(body, out_shape, args, spaces, out_spaces, aliases=None, scratch=(), flops=0, limit=4, nbytes=0):
    spec = {
        "v": pl.BlockSpec(memory_space=pltpu.VMEM),
        "s": pl.BlockSpec(memory_space=pltpu.SMEM),
        "h": pl.BlockSpec(memory_space=pl.ANY),
    }
    args = [
        arg if space == "s" else pltpu.with_memory_space_constraint(arg, pltpu.VMEM if space == "v" else pltpu.HBM)
        for arg, space in zip(args, spaces)
    ]
    return pl.pallas_call(
        body,
        out_shape=out_shape,
        in_specs=[spec[space] for space in spaces],
        out_specs=[spec[space] for space in out_spaces],
        input_output_aliases=aliases or {},
        scratch_shapes=list(scratch),
        compiler_params=pltpu.CompilerParams(vmem_limit_bytes=limit * 1024 * 1024),
        cost_estimate=pl.CostEstimate(flops=flops, bytes_accessed=nbytes, transcendentals=0),
    )(*args)


def position():
    me_y, last_y = lax.axis_index("gy"), lax.axis_size("gy") - 1
    inside = jnp.where((me_y > 0) & (me_y < last_y), 1, 0)
    return lax.rem(lax.axis_index("gx"), 2), lax.rem(me_y, 2), inside, lax.axis_index("gz")


def tile_iota(dim):
    return lax.broadcasted_iota(jnp.int32, (8, LANES), dim)


def column_tile(place):
    high = place[3] == 0
    offset = pl.multiple_of(jnp.where(high, 512 - LANES, 0), LANES)
    return offset, jnp.where(high, LANES - 1, 0)


def pack_columns(read, offset, lane, out_ref):
    lanes = tile_iota(1)
    parts = []
    for t in range(8):
        columns = jnp.zeros((8, LANES), jnp.float32)
        for i in range(16):
            moved = pltpu.roll(read(i, t, offset), (16 * t + i - lane) & (LANES - 1), 1)
            columns = jnp.where(lanes == 16 * t + i, moved, columns)
        parts.append(columns)
    while len(parts) > 1:
        parts = [one + other for one, other in zip(parts[::2], parts[1::2])]
    out_ref[...] = parts[0]


def sides(place):
    even_x = place[0] == 0
    even_y = place[1] == 0
    planes = jnp.where(even_x, 15, 0), jnp.where(even_x, 0, 15)
    rows = jnp.where(even_y, 63, 0), jnp.where(even_y, 0, 63)
    tiles = [pl.multiple_of(jnp.where(even_y, high, low), 8) for high, low in ((56, 0), (0, 56))]
    return planes, rows, tiles


def write_side_faces(rows_at, tile_at, place, ya, yb, zface):
    for n, face in enumerate((ya, yb)):
        values = [rows_at(n, i) for i in range(16)]
        for i in range(16):
            face[i : i + 1, :] = values[i]
    offset, lane = column_tile(place)
    pack_columns(lambda i, t, off: tile_at(i, t), offset, lane, zface)


FACES = [(64, 512), (64, 512), (16, 512), (16, 512), (8, LANES)]


def first_faces(rhs_hbm, xa, xb, ya, yb, zface, rows_a, rows_b, column, sem):
    place = position()
    planes, rows, tiles = sides(place)
    offset, _ = column_tile(place)
    copies = [
        pltpu.make_async_copy(rhs_hbm.at[:, :, pl.ds(offset, LANES)], column, sem.at[0]),
        pltpu.make_async_copy(rhs_hbm.at[:, pl.ds(tiles[0], 8), :], rows_a, sem.at[1]),
        pltpu.make_async_copy(rhs_hbm.at[:, pl.ds(tiles[1], 8), :], rows_b, sem.at[2]),
        pltpu.make_async_copy(rhs_hbm.at[planes[0]], xa, sem.at[3]),
        pltpu.make_async_copy(rhs_hbm.at[planes[1]], xb, sem.at[4]),
    ]
    for copy in copies:
        copy.start()
    for copy in copies[:3]:
        copy.wait()
    held = rows_a, rows_b
    write_side_faces(
        lambda n, i: held[n][i, pl.ds(lax.rem(rows[n], 8), 1), :],
        lambda i, t: column[i, 8 * t : 8 * t + 8, :],
        place, ya, yb, zface,
    )
    for copy in copies[3:]:
        copy.wait()


def row_of_tiles(ref, i, t):
    return [ref[i, 8 * t : 8 * t + 8, LANES * j : LANES * j + LANES] for j in range(4)]


def plane_terms(values_ref, diagonal, velocity_ref, i, emit):
    row, lane = tile_iota(0), tile_iota(1)
    first_row, last_row, first_lane, last_lane = row == 0, row == 7, lane == 0, lane == LANES - 1
    zero = jnp.zeros((8, LANES), jnp.float32)
    below = [zero] * 4
    here = row_of_tiles(values_ref, i, 0)
    for t in range(8):
        rows = slice(8 * t, 8 * t + 8)
        above = row_of_tiles(values_ref, i, t + 1) if t < 7 else [zero] * 4
        for j in range(4):
            lanes = slice(LANES * j, LANES * j + LANES)
            plus_y = pltpu.roll(jnp.where(first_row, above[j], here[j]), 7, 0)
            minus_y = pltpu.roll(jnp.where(last_row, below[j], here[j]), 1, 0)
            plus_z = pltpu.roll(jnp.where(first_lane, here[j + 1] if j < 3 else zero, here[j]), LANES - 1, 1)
            minus_z = pltpu.roll(jnp.where(last_lane, here[j - 1] if j > 0 else zero, here[j]), 1, 1)
            vx = velocity_ref[0, i, rows, lanes]
            if i == 0:
                plus_x = values_ref[i + 1, rows, lanes]
                beside = plus_x - vx * plus_x
            elif i == 15:
                minus_x = values_ref[i - 1, rows, lanes]
                beside = minus_x + vx * minus_x
            else:
                plus_x = values_ref[i + 1, rows, lanes]
                minus_x = values_ref[i - 1, rows, lanes]
                beside = plus_x - vx * (plus_x - minus_x) + minus_x
            beside = beside + (plus_y - velocity_ref[1, i, rows, lanes] * (plus_y - minus_y)) + minus_y
            beside = beside + (plus_z - velocity_ref[2, i, rows, lanes] * (plus_z - minus_z)) + minus_z
            emit(i, rows, lanes, here[j], diagonal(i, rows, lanes) * here[j] - beside)
        below, here = here, above


def first_main(rhs_ref, reaction_ref, velocity_ref, r_ref, d_ref, diag_ref, xa_c, xb_c, ya_c, yb_c, z_c):
    place = position()
    factor, gain = step_factors(0)

    def diagonal(i, rows, lanes):
        value = 6.0 + reaction_ref[i, rows, lanes]
        diag_ref[i, rows, lanes] = value
        return value

    def emit(i, rows, lanes, here, applied):
        residual = here - applied * (1.0 / centre)
        r_ref[i, rows, lanes] = residual
        d_ref[i, rows, lanes] = (factor / centre) * here + gain * residual

    for i in range(16):
        plane_terms(rhs_ref, diagonal, velocity_ref, i, emit)
    planes, _, tiles = sides(place)
    sign_x = jnp.where(place[0] == 0, -1.0, 1.0)
    sign_y = jnp.where(place[1] == 0, -1.0, 1.0)
    inside = (place[2] > 0).astype(jnp.float32)
    row = lax.broadcasted_iota(jnp.int32, (8, 512), 0)
    xa_c[...] = 1.0 + sign_x * velocity_ref[0, planes[0]]
    xb_c[...] = 1.0 - sign_x * velocity_ref[0, planes[1]]
    row_a = jnp.where(place[1] == 0, 7, 0)
    for i in range(16):
        own_a = 1.0 + sign_y * velocity_ref[1, i, pl.ds(tiles[0], 8), :]
        own_b = (1.0 - sign_y * velocity_ref[1, i, pl.ds(tiles[1], 8), :]) * inside
        ya_c[i] = jnp.where(row == row_a, own_a, 0.0)
        yb_c[i] = jnp.where(row == 7 - row_a, own_b, 0.0)
    offset, lane = column_tile(place)
    sign = jnp.where(place[3] == 0, -1.0, 1.0)
    pack_columns(
        lambda i, t, off: 1.0 + sign * velocity_ref[2, i, 8 * t : 8 * t + 8, pl.ds(off, LANES)], offset, lane, z_c
    )


def held(ref):
    return lambda i, rows, lanes: ref[i, rows, lanes]


def main(factor, gain, s_scale, d_ref, r_ref, s_ref, diag_ref, velocity_ref, r_out, d_out, s_out):
    def emit(i, rows, lanes, here, applied):
        residual = r_ref[i, rows, lanes] - applied
        r_out[i, rows, lanes] = residual
        before = s_ref[i, rows, lanes]
        s_out[i, rows, lanes] = (before if s_scale is None else before * s_scale) + here
        d_out[i, rows, lanes] = factor * here + gain * residual

    for i in range(16):
        plane_terms(d_ref, held(diag_ref), velocity_ref, i, emit)


def last_main(d_ref, r_ref, s_ref, diag_ref, velocity_ref, r_out, s_out):
    def emit(i, rows, lanes, here, applied):
        r_out[i, rows, lanes] = r_ref[i, rows, lanes] - applied
        s_out[i, rows, lanes] = s_ref[i, rows, lanes] + here

    for i in range(16):
        plane_terms(d_ref, held(diag_ref), velocity_ref, i, emit)


def correct(gain, place, scale, halos, coefs, r_ref, d_ref, ends, inner):
    hxa, hxb, hya, hyb, hz = halos
    xa_c, xb_c, ya_c, yb_c, z_c = coefs
    planes, _, tiles = sides(place)
    which = ([0, 15] if ends else []) + (list(range(1, 15)) if inner else [])

    def term(coef, halo):
        return coef * halo if scale is None else coef * halo * scale

    def add(places, changes):
        new_r = [r_ref[at] + change for at, change in zip(places, changes)]
        if d_ref is not None:
            new_d = [d_ref[at] + gain * change for at, change in zip(places, changes)]
        for n, at in enumerate(places):
            r_ref[at] = new_r[n]
            if d_ref is not None:
                d_ref[at] = new_d[n]

    if ends:
        for t in range(0, 64, 16):
            rows = slice(t, t + 16)
            add([(planes[0], rows)], [term(xa_c[rows, :], hxa[rows, :])])
            add([(planes[1], rows)], [term(xb_c[rows, :], hxb[rows, :])])
    for first in range(0, len(which), 4):
        group = which[first : first + 4]
        for tile, coef, halo in ((tiles[0], ya_c, hya), (tiles[1], yb_c, hyb)):
            changes = [term(coef[i], jnp.broadcast_to(halo[i : i + 1, :], (8, 512))) for i in group]
            add([(i, pl.ds(tile, 8)) for i in group], changes)
    offset, lane = column_tile(place)
    lanes = tile_iota(1)
    packed = term(z_c[...], hz[...])
    for t in range(8):
        rows = slice(8 * t, 8 * t + 8)
        shifts = [(lane - i - 16 * t) & (LANES - 1) for i in which]
        moved = [jnp.where(lanes == lane, pltpu.roll(packed, shift, 1), 0.0) for shift in shifts]
        add([(i, rows, pl.ds(offset, LANES)) for i in which], moved)


def fix_ends(gain, scale, *refs):
    halos, coefs, (_, _), (r_ref, d_ref, xa, xb) = refs[:5], refs[5:10], refs[10:12], refs[12:]
    place = position()
    correct(gain, place, scale, halos, coefs, r_ref, d_ref, True, False)
    planes, _, _ = sides(place)
    xa[...] = d_ref[planes[0]]
    xb[...] = d_ref[planes[1]]


def fix_inner(gain, scale, *refs):
    (hya, hyb, hz), (ya_c, yb_c, z_c), (_, _), (r_ref, d_ref, ya, yb, zface) = refs[:3], refs[3:6], refs[6:8], refs[8:]
    place = position()
    halos, coefs = (None, None, hya, hyb, hz), (None, None, ya_c, yb_c, z_c)
    correct(gain, place, scale, halos, coefs, r_ref, d_ref, False, True)
    _, rows, _ = sides(place)
    offset, _ = column_tile(place)
    write_side_faces(
        lambda n, i: d_ref[i, pl.ds(rows[n], 1), :],
        lambda i, t: d_ref[i, 8 * t : 8 * t + 8, pl.ds(offset, LANES)],
        place, ya, yb, zface,
    )


def last_fix(*refs):
    halos, coefs = refs[:5], refs[5:10]
    _, r_ref, part_ref = refs[10:]
    correct(None, position(), None, halos, coefs, r_ref, None, True, True)

    def plane(i, total):
        for t in range(8):
            value = r_ref[i, 8 * t : 8 * t + 8, :]
            total = total + value * value
        return total

    total = lax.fori_loop(0, 16, plane, jnp.zeros((8, 512), jnp.float32), unroll=2)
    part_ref[...] = jnp.broadcast_to(jnp.sum(total).reshape(1, 1), part_ref.shape)


def save(held_ref, out_hbm, sem):
    copy = pltpu.make_async_copy(held_ref, out_hbm, sem)
    copy.start()
    copy.wait()


def finish(cells, got_ref, out_ref):
    total = jnp.sum(got_ref[...], axis=0, keepdims=True)
    out_ref[...] = jnp.sqrt(total / cells + 1e-06)


def local(right_side, reaction, velocity):
    gx, gy, gz = lax.axis_size("gx"), lax.axis_size("gy"), lax.axis_size("gz")
    shape = right_side.shape
    block = in_vmem(shape)
    face_shapes = [in_vmem(face) for face in FACES]

    def pairs(n, first):
        step = [1 - 2 * (i % 2) if first else 2 * (i % 2) - 1 for i in range(n)]
        return [(i, (i + step[i]) % n) for i in range(n)]

    def exchange_x(xa, xb):
        far = lax.ppermute(xb, "gx", pairs(gx, False))
        return [lax.ppermute(xa, "gx", pairs(gx, True)), far]

    def exchange_sides(ya, yb, zface):
        far = lax.ppermute(yb, "gy", pairs(gy, False))
        across = lax.ppermute(zface, "gz", pairs(gz, True))
        return [lax.ppermute(ya, "gy", pairs(gy, True)), far, across]

    rows = pltpu.VMEM((16, 8, 512), jnp.float32)
    faces = call(
        first_faces,
        face_shapes,
        [right_side],
        "h",
        "vvvvv",
        scratch=[rows, rows, pltpu.VMEM((16, 64, LANES), jnp.float32), pltpu.SemaphoreType.DMA((5,))],
        flops=100 * COST,
    )
    halos = exchange_x(*faces[:2]) + exchange_sides(*faces[2:])
    r, d, diag, *coefs = call(
        first_main,
        [block, block, block]
        + [in_vmem(s) for s in [(64, 512), (64, 512), (16, 8, 512), (16, 8, 512), (8, LANES)]],
        [right_side, reaction, velocity],
        "vvv",
        "v" * 8,
        flops=COST,
    )
    s = right_side
    for iteration in range(ITERS):
        if iteration > 0:
            if iteration + 1 < ITERS:
                r, d, s = call(
                    functools.partial(main, *step_factors(iteration), 1.0 / centre if iteration == 1 else None),
                    [block] * 3,
                    [d, r, s, diag, velocity],
                    "vvvvv",
                    "vvv",
                    flops=COST,
                )
            else:
                r, s = call(last_main, [block, block], [d, r, s, diag, velocity], "vvvvv", "vv", flops=COST)
        if iteration + 1 < ITERS:
            gain = step_factors(iteration)[1]
            scale = 1.0 / centre if iteration == 0 else None
            r, d, *x_faces = call(
                functools.partial(fix_ends, gain, scale),
                [block, block] + face_shapes[:2],
                [*halos, *coefs, r, d],
                "v" * 12,
                "v" * 4,
                aliases={10: 0, 11: 1},
            )
            next_halos = exchange_x(*x_faces)
            r, d, *side_faces = call(
                functools.partial(fix_inner, gain, scale),
                [block, block] + face_shapes[2:],
                [*halos[2:], *coefs[2:], r, d],
                "v" * 8,
                "v" * 5,
                aliases={6: 0, 7: 1},
            )
            halos = next_halos + exchange_sides(*side_faces)
    devices = gx * gy * gz
    residual, part = call(
        last_fix, [block, in_vmem((devices, LANES))], [*halos, *coefs, r], "v" * 11, "vv", aliases={10: 0}
    )
    solution_out = call(
        save, [pltpu.HBM(shape, jnp.float32)], [s], "v", "h", scratch=[pltpu.SemaphoreType.DMA], flops=COST
    )[0]
    part = part.reshape(devices, 1, LANES)
    got = lax.all_to_all(part, ("gx", "gy", "gz"), 0, 0, tiled=True).reshape(devices, LANES)
    cells = shape[0] * shape[1] * shape[2] * devices
    norm = call(functools.partial(finish, cells), [in_vmem((1, LANES))], [got], "v", "v")[0]
    return solution_out, residual, norm[0, 0]


def solution(mesh):
    return jax.shard_map(
        local,
        mesh=mesh,
        in_specs=(P("gx", "gy", "gz"), P("gx", "gy", "gz"), P(None, "gx", "gy", "gz")),
        out_specs=(P("gx", "gy", "gz"), P("gx", "gy", "gz"), P()),
        check_vma=False,
    )
```

```python
import functools

import jax
import jax.numpy as jnp
from jax import lax
from jax.experimental import pallas as pl
from jax.experimental.pallas import tpu as pltpu
from jax.sharding import PartitionSpec as P


ITERS = 5
LANES = 128
COST = 10**8

centre = 7.25
half_width = 6.75


def chebyshev_weights(count):
    ratio_value = centre / half_width
    weights = [1.0 / ratio_value]
    for _ in range(count):
        weights.append(1.0 / (2.0 * ratio_value - weights[-1]))
    return weights


def step_factors(iteration):
    weights = chebyshev_weights(ITERS)
    return weights[iteration + 1] * weights[iteration], 2.0 * weights[iteration + 1] / half_width


def in_vmem(shape):
    return pltpu.VMEM(shape, jnp.float32)


def call(body, out_shape, args, spaces, out_spaces, aliases=None, scratch=(), flops=0, limit=4, nbytes=0):
    spec = {
        "v": pl.BlockSpec(memory_space=pltpu.VMEM),
        "s": pl.BlockSpec(memory_space=pltpu.SMEM),
        "h": pl.BlockSpec(memory_space=pl.ANY),
    }
    args = [
        arg if space == "s" else pltpu.with_memory_space_constraint(arg, pltpu.VMEM if space == "v" else pltpu.HBM)
        for arg, space in zip(args, spaces)
    ]
    return pl.pallas_call(
        body,
        out_shape=out_shape,
        in_specs=[spec[space] for space in spaces],
        out_specs=[spec[space] for space in out_spaces],
        input_output_aliases=aliases or {},
        scratch_shapes=list(scratch),
        compiler_params=pltpu.CompilerParams(vmem_limit_bytes=limit * 1024 * 1024),
        cost_estimate=pl.CostEstimate(flops=flops, bytes_accessed=nbytes, transcendentals=0),
    )(*args)


def position():
    me_y, last_y = lax.axis_index("gy"), lax.axis_size("gy") - 1
    inside = jnp.where((me_y > 0) & (me_y < last_y), 1, 0)
    return lax.rem(lax.axis_index("gx"), 2), lax.rem(me_y, 2), inside, lax.axis_index("gz")


def tile_iota(dim):
    return lax.broadcasted_iota(jnp.int32, (8, LANES), dim)


def column_tile(place):
    high = place[3] == 0
    offset = pl.multiple_of(jnp.where(high, 512 - LANES, 0), LANES)
    return offset, jnp.where(high, LANES - 1, 0)


def pack_columns(read, offset, lane, out_ref):
    lanes = tile_iota(1)
    parts = []
    for t in range(8):
        columns = jnp.zeros((8, LANES), jnp.float32)
        for i in range(16):
            moved = pltpu.roll(read(i, t, offset), (16 * t + i - lane) & (LANES - 1), 1)
            columns = jnp.where(lanes == 16 * t + i, moved, columns)
        parts.append(columns)
    while len(parts) > 1:
        parts = [one + other for one, other in zip(parts[::2], parts[1::2])]
    out_ref[...] = parts[0]


def sides(place):
    even_x = place[0] == 0
    even_y = place[1] == 0
    planes = jnp.where(even_x, 15, 0), jnp.where(even_x, 0, 15)
    rows = jnp.where(even_y, 63, 0), jnp.where(even_y, 0, 63)
    tiles = [pl.multiple_of(jnp.where(even_y, high, low), 8) for high, low in ((56, 0), (0, 56))]
    return planes, rows, tiles


def write_side_faces(rows_at, tile_at, place, ya, yb, zface):
    for n, face in enumerate((ya, yb)):
        values = [rows_at(n, i) for i in range(16)]
        for i in range(16):
            face[i : i + 1, :] = values[i]
    offset, lane = column_tile(place)
    pack_columns(lambda i, t, off: tile_at(i, t), offset, lane, zface)


FACES = [(64, 512), (64, 512), (16, 512), (16, 512), (8, LANES)]


def first_x_faces(rhs_hbm, xa, xb, sem):
    planes, _, _ = sides(position())
    copies = [
        pltpu.make_async_copy(rhs_hbm.at[planes[0]], xa, sem.at[0]),
        pltpu.make_async_copy(rhs_hbm.at[planes[1]], xb, sem.at[1]),
    ]
    for copy in copies:
        copy.start()
    for copy in copies:
        copy.wait()


def first_side_faces(rhs_ref, ya, yb, zface):
    place = position()
    _, rows, _ = sides(place)
    offset, _ = column_tile(place)
    write_side_faces(
        lambda n, i: rhs_ref[i, pl.ds(rows[n], 1), :],
        lambda i, t: rhs_ref[i, 8 * t : 8 * t + 8, pl.ds(offset, LANES)],
        place, ya, yb, zface,
    )


def row_of_tiles(ref, i, t):
    return [ref[i, 8 * t : 8 * t + 8, LANES * j : LANES * j + LANES] for j in range(4)]


def plane_terms(values_ref, diagonal, velocity_ref, i, emit):
    row, lane = tile_iota(0), tile_iota(1)
    first_row, last_row, first_lane, last_lane = row == 0, row == 7, lane == 0, lane == LANES - 1
    zero = jnp.zeros((8, LANES), jnp.float32)
    below = [zero] * 4
    here = row_of_tiles(values_ref, i, 0)
    for t in range(8):
        rows = slice(8 * t, 8 * t + 8)
        above = row_of_tiles(values_ref, i, t + 1) if t < 7 else [zero] * 4
        for j in range(4):
            lanes = slice(LANES * j, LANES * j + LANES)
            plus_y = pltpu.roll(jnp.where(first_row, above[j], here[j]), 7, 0)
            minus_y = pltpu.roll(jnp.where(last_row, below[j], here[j]), 1, 0)
            plus_z = pltpu.roll(jnp.where(first_lane, here[j + 1] if j < 3 else zero, here[j]), LANES - 1, 1)
            minus_z = pltpu.roll(jnp.where(last_lane, here[j - 1] if j > 0 else zero, here[j]), 1, 1)
            vx = velocity_ref[0, i, rows, lanes]
            if i == 0:
                plus_x = values_ref[i + 1, rows, lanes]
                beside = plus_x - vx * plus_x
            elif i == 15:
                minus_x = values_ref[i - 1, rows, lanes]
                beside = minus_x + vx * minus_x
            else:
                plus_x = values_ref[i + 1, rows, lanes]
                minus_x = values_ref[i - 1, rows, lanes]
                beside = plus_x - vx * (plus_x - minus_x) + minus_x
            beside = beside + (plus_y - velocity_ref[1, i, rows, lanes] * (plus_y - minus_y)) + minus_y
            beside = beside + (plus_z - velocity_ref[2, i, rows, lanes] * (plus_z - minus_z)) + minus_z
            emit(i, rows, lanes, here[j], diagonal(i, rows, lanes) * here[j] - beside)
        below, here = here, above


def first_main(rhs_ref, reaction_ref, velocity_ref, r_ref, d_ref, diag_ref, xa_c, xb_c, ya_c, yb_c, z_c):
    place = position()
    factor, gain = step_factors(0)

    def diagonal(i, rows, lanes):
        value = 6.0 + reaction_ref[i, rows, lanes]
        diag_ref[i, rows, lanes] = value
        return value

    def emit(i, rows, lanes, here, applied):
        residual = here - applied * (1.0 / centre)
        r_ref[i, rows, lanes] = residual
        d_ref[i, rows, lanes] = (factor / centre) * here + gain * residual

    for i in range(16):
        plane_terms(rhs_ref, diagonal, velocity_ref, i, emit)
    planes, _, tiles = sides(place)
    sign_x = jnp.where(place[0] == 0, -1.0, 1.0)
    sign_y = jnp.where(place[1] == 0, -1.0, 1.0)
    inside = (place[2] > 0).astype(jnp.float32)
    row = lax.broadcasted_iota(jnp.int32, (8, 512), 0)
    xa_c[...] = 1.0 + sign_x * velocity_ref[0, planes[0]]
    xb_c[...] = 1.0 - sign_x * velocity_ref[0, planes[1]]
    row_a = jnp.where(place[1] == 0, 7, 0)
    for i in range(16):
        own_a = 1.0 + sign_y * velocity_ref[1, i, pl.ds(tiles[0], 8), :]
        own_b = (1.0 - sign_y * velocity_ref[1, i, pl.ds(tiles[1], 8), :]) * inside
        ya_c[i] = jnp.where(row == row_a, own_a, 0.0)
        yb_c[i] = jnp.where(row == 7 - row_a, own_b, 0.0)
    offset, lane = column_tile(place)
    sign = jnp.where(place[3] == 0, -1.0, 1.0)
    pack_columns(
        lambda i, t, off: 1.0 + sign * velocity_ref[2, i, 8 * t : 8 * t + 8, pl.ds(off, LANES)], offset, lane, z_c
    )


def held(ref):
    return lambda i, rows, lanes: ref[i, rows, lanes]


def main(factor, gain, s_scale, d_ref, r_ref, s_ref, diag_ref, velocity_ref, r_out, d_out, s_out):
    def emit(i, rows, lanes, here, applied):
        residual = r_ref[i, rows, lanes] - applied
        r_out[i, rows, lanes] = residual
        before = s_ref[i, rows, lanes]
        s_out[i, rows, lanes] = (before if s_scale is None else before * s_scale) + here
        d_out[i, rows, lanes] = factor * here + gain * residual

    for i in range(16):
        plane_terms(d_ref, held(diag_ref), velocity_ref, i, emit)


def last_main(d_ref, r_ref, s_ref, diag_ref, velocity_ref, r_out, s_out):
    def emit(i, rows, lanes, here, applied):
        r_out[i, rows, lanes] = r_ref[i, rows, lanes] - applied
        s_out[i, rows, lanes] = s_ref[i, rows, lanes] + here

    for i in range(16):
        plane_terms(d_ref, held(diag_ref), velocity_ref, i, emit)


def correct(gain, place, scale, halos, coefs, r_ref, d_ref, ends, inner):
    hxa, hxb, hya, hyb, hz = halos
    xa_c, xb_c, ya_c, yb_c, z_c = coefs
    planes, _, tiles = sides(place)
    which = ([0, 15] if ends else []) + (list(range(1, 15)) if inner else [])

    def term(coef, halo):
        return coef * halo if scale is None else coef * halo * scale

    def add(places, changes):
        new_r = [r_ref[at] + change for at, change in zip(places, changes)]
        if d_ref is not None:
            new_d = [d_ref[at] + gain * change for at, change in zip(places, changes)]
        for n, at in enumerate(places):
            r_ref[at] = new_r[n]
            if d_ref is not None:
                d_ref[at] = new_d[n]

    if ends:
        for t in range(0, 64, 16):
            rows = slice(t, t + 16)
            add([(planes[0], rows)], [term(xa_c[rows, :], hxa[rows, :])])
            add([(planes[1], rows)], [term(xb_c[rows, :], hxb[rows, :])])
    for first in range(0, len(which), 4):
        group = which[first : first + 4]
        for tile, coef, halo in ((tiles[0], ya_c, hya), (tiles[1], yb_c, hyb)):
            changes = [term(coef[i], jnp.broadcast_to(halo[i : i + 1, :], (8, 512))) for i in group]
            add([(i, pl.ds(tile, 8)) for i in group], changes)
    offset, lane = column_tile(place)
    lanes = tile_iota(1)
    packed = term(z_c[...], hz[...])
    for t in range(8):
        rows = slice(8 * t, 8 * t + 8)
        shifts = [(lane - i - 16 * t) & (LANES - 1) for i in which]
        moved = [jnp.where(lanes == lane, pltpu.roll(packed, shift, 1), 0.0) for shift in shifts]
        add([(i, rows, pl.ds(offset, LANES)) for i in which], moved)


def fix_ends(gain, scale, *refs):
    halos, coefs, (_, _), (r_ref, d_ref, xa, xb) = refs[:5], refs[5:10], refs[10:12], refs[12:]
    place = position()
    correct(gain, place, scale, halos, coefs, r_ref, d_ref, True, False)
    planes, _, _ = sides(place)
    xa[...] = d_ref[planes[0]]
    xb[...] = d_ref[planes[1]]


def fix_inner(gain, scale, *refs):
    (hya, hyb, hz), (ya_c, yb_c, z_c), (_, _), (r_ref, d_ref, ya, yb, zface) = refs[:3], refs[3:6], refs[6:8], refs[8:]
    place = position()
    halos, coefs = (None, None, hya, hyb, hz), (None, None, ya_c, yb_c, z_c)
    correct(gain, place, scale, halos, coefs, r_ref, d_ref, False, True)
    _, rows, _ = sides(place)
    offset, _ = column_tile(place)
    write_side_faces(
        lambda n, i: d_ref[i, pl.ds(rows[n], 1), :],
        lambda i, t: d_ref[i, 8 * t : 8 * t + 8, pl.ds(offset, LANES)],
        place, ya, yb, zface,
    )


def last_fix(*refs):
    halos, coefs = refs[:5], refs[5:10]
    _, r_ref, part_ref = refs[10:]
    correct(None, position(), None, halos, coefs, r_ref, None, True, True)

    def plane(i, total):
        for t in range(8):
            value = r_ref[i, 8 * t : 8 * t + 8, :]
            total = total + value * value
        return total

    total = lax.fori_loop(0, 16, plane, jnp.zeros((8, 512), jnp.float32), unroll=2)
    part_ref[...] = jnp.broadcast_to(jnp.sum(total).reshape(1, 1), part_ref.shape)


def save(held_ref, out_hbm, sem):
    copy = pltpu.make_async_copy(held_ref, out_hbm, sem)
    copy.start()
    copy.wait()


def finish(cells, got_ref, out_ref):
    total = jnp.sum(got_ref[...], axis=0, keepdims=True)
    out_ref[...] = jnp.sqrt(total / cells + 1e-06)


def local(right_side, reaction, velocity):
    gx, gy, gz = lax.axis_size("gx"), lax.axis_size("gy"), lax.axis_size("gz")
    shape = right_side.shape
    block = in_vmem(shape)
    face_shapes = [in_vmem(face) for face in FACES]

    def pairs(n, first):
        step = [1 - 2 * (i % 2) if first else 2 * (i % 2) - 1 for i in range(n)]
        return [(i, (i + step[i]) % n) for i in range(n)]

    def exchange_x(xa, xb):
        far = lax.ppermute(xb, "gx", pairs(gx, False))
        return [lax.ppermute(xa, "gx", pairs(gx, True)), far]

    def exchange_sides(ya, yb, zface):
        far = lax.ppermute(yb, "gy", pairs(gy, False))
        across = lax.ppermute(zface, "gz", pairs(gz, True))
        return [lax.ppermute(ya, "gy", pairs(gy, True)), far, across]

    x_faces = call(
        first_x_faces,
        face_shapes[:2],
        [right_side],
        "h",
        "vv",
        scratch=[pltpu.SemaphoreType.DMA((2,))],
        flops=100 * COST,
    )
    halos = exchange_x(*x_faces)
    side_faces = call(first_side_faces, face_shapes[2:], [right_side], "v", "vvv")
    halos += exchange_sides(*side_faces)
    r, d, diag, *coefs = call(
        first_main,
        [block, block, block]
        + [in_vmem(s) for s in [(64, 512), (64, 512), (16, 8, 512), (16, 8, 512), (8, LANES)]],
        [right_side, reaction, velocity],
        "vvv",
        "v" * 8,
        flops=COST,
    )
    s = right_side
    for iteration in range(ITERS):
        if iteration > 0:
            if iteration + 1 < ITERS:
                r, d, s = call(
                    functools.partial(main, *step_factors(iteration), 1.0 / centre if iteration == 1 else None),
                    [block] * 3,
                    [d, r, s, diag, velocity],
                    "vvvvv",
                    "vvv",
                    flops=COST,
                )
            else:
                r, s = call(last_main, [block, block], [d, r, s, diag, velocity], "vvvvv", "vv", flops=COST)
        if iteration + 1 < ITERS:
            gain = step_factors(iteration)[1]
            scale = 1.0 / centre if iteration == 0 else None
            r, d, *x_faces = call(
                functools.partial(fix_ends, gain, scale),
                [block, block] + face_shapes[:2],
                [*halos, *coefs, r, d],
                "v" * 12,
                "v" * 4,
                aliases={10: 0, 11: 1},
            )
            next_halos = exchange_x(*x_faces)
            r, d, *side_faces = call(
                functools.partial(fix_inner, gain, scale),
                [block, block] + face_shapes[2:],
                [*halos[2:], *coefs[2:], r, d],
                "v" * 8,
                "v" * 5,
                aliases={6: 0, 7: 1},
            )
            halos = next_halos + exchange_sides(*side_faces)
    devices = gx * gy * gz
    residual, part = call(
        last_fix, [block, in_vmem((devices, LANES))], [*halos, *coefs, r], "v" * 11, "vv", aliases={10: 0}
    )
    solution_out = call(
        save, [pltpu.HBM(shape, jnp.float32)], [s], "v", "h", scratch=[pltpu.SemaphoreType.DMA], flops=COST
    )[0]
    part = part.reshape(devices, 1, LANES)
    got = lax.all_to_all(part, ("gx", "gy", "gz"), 0, 0, tiled=True).reshape(devices, LANES)
    cells = shape[0] * shape[1] * shape[2] * devices
    norm = call(functools.partial(finish, cells), [in_vmem((1, LANES))], [got], "v", "v")[0]
    return solution_out, residual, norm[0, 0]


def solution(mesh):
    return jax.shard_map(
        local,
        mesh=mesh,
        in_specs=(P("gx", "gy", "gz"), P("gx", "gy", "gz"), P(None, "gx", "gy", "gz")),
        out_specs=(P("gx", "gy", "gz"), P("gx", "gy", "gz"), P()),
        check_vma=False,
    )
```

```python
import functools

import jax
import jax.numpy as jnp
from jax import lax
from jax.experimental import pallas as pl
from jax.experimental.pallas import tpu as pltpu
from jax.sharding import PartitionSpec as P


ITERS = 5
LANES = 128
COST = 10**8

centre = 7.25
half_width = 6.75


def chebyshev_weights(count):
    ratio_value = centre / half_width
    weights = [1.0 / ratio_value]
    for _ in range(count):
        weights.append(1.0 / (2.0 * ratio_value - weights[-1]))
    return weights


def step_factors(iteration):
    weights = chebyshev_weights(ITERS)
    return weights[iteration + 1] * weights[iteration], 2.0 * weights[iteration + 1] / half_width


def in_vmem(shape):
    return pltpu.VMEM(shape, jnp.float32)


def call(body, out_shape, args, spaces, out_spaces, aliases=None, scratch=(), flops=0, limit=4, nbytes=0):
    spec = {
        "v": pl.BlockSpec(memory_space=pltpu.VMEM),
        "s": pl.BlockSpec(memory_space=pltpu.SMEM),
        "h": pl.BlockSpec(memory_space=pl.ANY),
    }
    args = [
        arg if space == "s" else pltpu.with_memory_space_constraint(arg, pltpu.VMEM if space == "v" else pltpu.HBM)
        for arg, space in zip(args, spaces)
    ]
    return pl.pallas_call(
        body,
        out_shape=out_shape,
        in_specs=[spec[space] for space in spaces],
        out_specs=[spec[space] for space in out_spaces],
        input_output_aliases=aliases or {},
        scratch_shapes=list(scratch),
        compiler_params=pltpu.CompilerParams(vmem_limit_bytes=limit * 1024 * 1024),
        cost_estimate=pl.CostEstimate(flops=flops, bytes_accessed=nbytes, transcendentals=0),
    )(*args)


def position():
    me_y, last_y = lax.axis_index("gy"), lax.axis_size("gy") - 1
    inside = jnp.where((me_y > 0) & (me_y < last_y), 1, 0)
    return lax.rem(lax.axis_index("gx"), 2), lax.rem(me_y, 2), inside, lax.axis_index("gz")


def tile_iota(dim):
    return lax.broadcasted_iota(jnp.int32, (8, LANES), dim)


def column_tile(place):
    high = place[3] == 0
    offset = pl.multiple_of(jnp.where(high, 512 - LANES, 0), LANES)
    return offset, jnp.where(high, LANES - 1, 0)


def pack_columns(read, offset, lane, out_ref):
    lanes = tile_iota(1)
    parts = []
    for t in range(8):
        columns = jnp.zeros((8, LANES), jnp.float32)
        for i in range(16):
            moved = pltpu.roll(read(i, t, offset), (16 * t + i - lane) & (LANES - 1), 1)
            columns = jnp.where(lanes == 16 * t + i, moved, columns)
        parts.append(columns)
    while len(parts) > 1:
        parts = [one + other for one, other in zip(parts[::2], parts[1::2])]
    out_ref[...] = parts[0]


def sides(place):
    even_x = place[0] == 0
    even_y = place[1] == 0
    planes = jnp.where(even_x, 15, 0), jnp.where(even_x, 0, 15)
    rows = jnp.where(even_y, 63, 0), jnp.where(even_y, 0, 63)
    tiles = [pl.multiple_of(jnp.where(even_y, high, low), 8) for high, low in ((56, 0), (0, 56))]
    return planes, rows, tiles


def write_side_faces(rows_at, tile_at, place, ya, yb, zface):
    for n, face in enumerate((ya, yb)):
        values = [rows_at(n, i) for i in range(16)]
        for i in range(16):
            face[i : i + 1, :] = values[i]
    offset, lane = column_tile(place)
    pack_columns(lambda i, t, off: tile_at(i, t), offset, lane, zface)


FACES = [(64, 512), (64, 512), (16, 512), (16, 512), (8, LANES)]


def first_x_faces(rhs_hbm, xa, xb, sem):
    planes, _, _ = sides(position())
    copies = [
        pltpu.make_async_copy(rhs_hbm.at[planes[0]], xa, sem.at[0]),
        pltpu.make_async_copy(rhs_hbm.at[planes[1]], xb, sem.at[1]),
    ]
    for copy in copies:
        copy.start()
    for copy in copies:
        copy.wait()


def first_side_faces(rhs_ref, ya, yb, zface):
    place = position()
    _, rows, _ = sides(place)
    offset, _ = column_tile(place)
    write_side_faces(
        lambda n, i: rhs_ref[i, pl.ds(rows[n], 1), :],
        lambda i, t: rhs_ref[i, 8 * t : 8 * t + 8, pl.ds(offset, LANES)],
        place, ya, yb, zface,
    )


def row_of_tiles(ref, i, t):
    return [ref[i, 8 * t : 8 * t + 8, LANES * j : LANES * j + LANES] for j in range(4)]


def plane_terms(values_ref, diagonal, velocity_ref, i, emit):
    row, lane = tile_iota(0), tile_iota(1)
    first_row, last_row, first_lane, last_lane = row == 0, row == 7, lane == 0, lane == LANES - 1
    zero = jnp.zeros((8, LANES), jnp.float32)
    below = [zero] * 4
    here = row_of_tiles(values_ref, i, 0)
    for t in range(8):
        rows = slice(8 * t, 8 * t + 8)
        above = row_of_tiles(values_ref, i, t + 1) if t < 7 else [zero] * 4
        for j in range(4):
            lanes = slice(LANES * j, LANES * j + LANES)
            plus_y = pltpu.roll(jnp.where(first_row, above[j], here[j]), 7, 0)
            minus_y = pltpu.roll(jnp.where(last_row, below[j], here[j]), 1, 0)
            plus_z = pltpu.roll(jnp.where(first_lane, here[j + 1] if j < 3 else zero, here[j]), LANES - 1, 1)
            minus_z = pltpu.roll(jnp.where(last_lane, here[j - 1] if j > 0 else zero, here[j]), 1, 1)
            vx = velocity_ref[0, i, rows, lanes]
            if i == 0:
                plus_x = values_ref[i + 1, rows, lanes]
                beside = plus_x - vx * plus_x
            elif i == 15:
                minus_x = values_ref[i - 1, rows, lanes]
                beside = minus_x + vx * minus_x
            else:
                plus_x = values_ref[i + 1, rows, lanes]
                minus_x = values_ref[i - 1, rows, lanes]
                beside = plus_x - vx * (plus_x - minus_x) + minus_x
            beside = beside + (plus_y - velocity_ref[1, i, rows, lanes] * (plus_y - minus_y)) + minus_y
            beside = beside + (plus_z - velocity_ref[2, i, rows, lanes] * (plus_z - minus_z)) + minus_z
            emit(i, rows, lanes, here[j], diagonal(i, rows, lanes) * here[j] - beside)
        below, here = here, above


def first_main(rhs_ref, reaction_ref, velocity_ref, r_ref, d_ref, diag_ref, xa_c, xb_c, ya_c, yb_c, z_c):
    place = position()
    factor, gain = step_factors(0)

    def diagonal(i, rows, lanes):
        value = 6.0 + reaction_ref[i, rows, lanes]
        diag_ref[i, rows, lanes] = value
        return value

    def emit(i, rows, lanes, here, applied):
        residual = here - applied * (1.0 / centre)
        r_ref[i, rows, lanes] = residual
        d_ref[i, rows, lanes] = (factor / centre) * here + gain * residual

    for i in range(16):
        plane_terms(rhs_ref, diagonal, velocity_ref, i, emit)
    planes, _, tiles = sides(place)
    sign_x = jnp.where(place[0] == 0, -1.0, 1.0)
    sign_y = jnp.where(place[1] == 0, -1.0, 1.0)
    inside = (place[2] > 0).astype(jnp.float32)
    row = lax.broadcasted_iota(jnp.int32, (8, 512), 0)
    xa_c[...] = 1.0 + sign_x * velocity_ref[0, planes[0]]
    xb_c[...] = 1.0 - sign_x * velocity_ref[0, planes[1]]
    row_a = jnp.where(place[1] == 0, 7, 0)
    for i in range(16):
        own_a = 1.0 + sign_y * velocity_ref[1, i, pl.ds(tiles[0], 8), :]
        own_b = (1.0 - sign_y * velocity_ref[1, i, pl.ds(tiles[1], 8), :]) * inside
        ya_c[i] = jnp.where(row == row_a, own_a, 0.0)
        yb_c[i] = jnp.where(row == 7 - row_a, own_b, 0.0)
    offset, lane = column_tile(place)
    sign = jnp.where(place[3] == 0, -1.0, 1.0)
    pack_columns(
        lambda i, t, off: 1.0 + sign * velocity_ref[2, i, 8 * t : 8 * t + 8, pl.ds(off, LANES)], offset, lane, z_c
    )


def held(ref):
    return lambda i, rows, lanes: ref[i, rows, lanes]


def main(factor, gain, s_scale, d_ref, r_ref, s_ref, diag_ref, velocity_ref, r_out, d_out, s_out):
    def emit(i, rows, lanes, here, applied):
        residual = r_ref[i, rows, lanes] - applied
        r_out[i, rows, lanes] = residual
        before = s_ref[i, rows, lanes]
        s_out[i, rows, lanes] = (before if s_scale is None else before * s_scale) + here
        d_out[i, rows, lanes] = factor * here + gain * residual

    for i in range(16):
        plane_terms(d_ref, held(diag_ref), velocity_ref, i, emit)


def last_main(d_ref, r_ref, s_ref, diag_ref, velocity_ref, r_out, s_out):
    def emit(i, rows, lanes, here, applied):
        r_out[i, rows, lanes] = r_ref[i, rows, lanes] - applied
        s_out[i, rows, lanes] = s_ref[i, rows, lanes] + here

    for i in range(16):
        plane_terms(d_ref, held(diag_ref), velocity_ref, i, emit)


def correct(gain, place, scale, halos, coefs, r_ref, d_ref, ends, inner):
    hxa, hxb, hya, hyb, hz = halos
    xa_c, xb_c, ya_c, yb_c, z_c = coefs
    planes, _, tiles = sides(place)
    which = ([0, 15] if ends else []) + (list(range(1, 15)) if inner else [])

    def term(coef, halo):
        return coef * halo if scale is None else coef * halo * scale

    def add(places, changes):
        new_r = [r_ref[at] + change for at, change in zip(places, changes)]
        if d_ref is not None:
            new_d = [d_ref[at] + gain * change for at, change in zip(places, changes)]
        for n, at in enumerate(places):
            r_ref[at] = new_r[n]
            if d_ref is not None:
                d_ref[at] = new_d[n]

    if ends:
        for t in range(0, 64, 16):
            rows = slice(t, t + 16)
            add([(planes[0], rows)], [term(xa_c[rows, :], hxa[rows, :])])
            add([(planes[1], rows)], [term(xb_c[rows, :], hxb[rows, :])])
    for first in range(0, len(which), 4):
        group = which[first : first + 4]
        for tile, coef, halo in ((tiles[0], ya_c, hya), (tiles[1], yb_c, hyb)):
            changes = [term(coef[i], jnp.broadcast_to(halo[i : i + 1, :], (8, 512))) for i in group]
            add([(i, pl.ds(tile, 8)) for i in group], changes)
    offset, lane = column_tile(place)
    lanes = tile_iota(1)
    packed = term(z_c[...], hz[...])
    for t in range(8):
        rows = slice(8 * t, 8 * t + 8)
        shifts = [(lane - i - 16 * t) & (LANES - 1) for i in which]
        moved = [jnp.where(lanes == lane, pltpu.roll(packed, shift, 1), 0.0) for shift in shifts]
        add([(i, rows, pl.ds(offset, LANES)) for i in which], moved)


def fix_ends(gain, scale, *refs):
    halos, coefs, (_, _), (r_ref, d_ref, xa, xb) = refs[:5], refs[5:10], refs[10:12], refs[12:]
    place = position()
    correct(gain, place, scale, halos, coefs, r_ref, d_ref, True, False)
    planes, _, _ = sides(place)
    xa[...] = d_ref[planes[0]]
    xb[...] = d_ref[planes[1]]


def fix_inner(gain, scale, *refs):
    (hya, hyb, hz), (ya_c, yb_c, z_c), (_, _), (r_ref, d_ref, ya, yb, zface) = refs[:3], refs[3:6], refs[6:8], refs[8:]
    place = position()
    halos, coefs = (None, None, hya, hyb, hz), (None, None, ya_c, yb_c, z_c)
    correct(gain, place, scale, halos, coefs, r_ref, d_ref, False, True)
    _, rows, _ = sides(place)
    offset, _ = column_tile(place)
    write_side_faces(
        lambda n, i: d_ref[i, pl.ds(rows[n], 1), :],
        lambda i, t: d_ref[i, 8 * t : 8 * t + 8, pl.ds(offset, LANES)],
        place, ya, yb, zface,
    )


def last_fix(*refs):
    halos, coefs = refs[:5], refs[5:10]
    _, r_ref, part_ref = refs[10:]
    correct(None, position(), None, halos, coefs, r_ref, None, True, True)

    totals = [jnp.zeros((8, 512), jnp.float32)] * 4
    for i in range(16):
        for t in range(8):
            value = r_ref[i, 8 * t : 8 * t + 8, :]
            totals[t % 4] = totals[t % 4] + value * value
    total = (totals[0] + totals[1]) + (totals[2] + totals[3])
    lanes = (total[:, :128] + total[:, 128:256]) + (total[:, 256:384] + total[:, 384:])
    part_ref[...] = jnp.broadcast_to(jnp.sum(lanes, axis=0, keepdims=True), part_ref.shape)


def save(held_ref, out_hbm, sem):
    copy = pltpu.make_async_copy(held_ref, out_hbm, sem)
    copy.start()
    copy.wait()


def finish(cells, got_ref, out_ref):
    total = jnp.sum(jnp.sum(got_ref[...], axis=0, keepdims=True), axis=1, keepdims=True)
    out_ref[...] = jnp.broadcast_to(jnp.sqrt(total / cells + 1e-06), out_ref.shape)


def local(right_side, reaction, velocity):
    gx, gy, gz = lax.axis_size("gx"), lax.axis_size("gy"), lax.axis_size("gz")
    shape = right_side.shape
    block = in_vmem(shape)
    face_shapes = [in_vmem(face) for face in FACES]

    def pairs(n, first):
        step = [1 - 2 * (i % 2) if first else 2 * (i % 2) - 1 for i in range(n)]
        return [(i, (i + step[i]) % n) for i in range(n)]

    def exchange_x(xa, xb):
        far = lax.ppermute(xb, "gx", pairs(gx, False))
        return [lax.ppermute(xa, "gx", pairs(gx, True)), far]

    def exchange_sides(ya, yb, zface):
        far = lax.ppermute(yb, "gy", pairs(gy, False))
        across = lax.ppermute(zface, "gz", pairs(gz, True))
        return [lax.ppermute(ya, "gy", pairs(gy, True)), far, across]

    x_faces = call(
        first_x_faces,
        face_shapes[:2],
        [right_side],
        "h",
        "vv",
        scratch=[pltpu.SemaphoreType.DMA((2,))],
        flops=100 * COST,
    )
    halos = exchange_x(*x_faces)
    side_faces = call(first_side_faces, face_shapes[2:], [right_side], "v", "vvv")
    halos += exchange_sides(*side_faces)
    r, d, diag, *coefs = call(
        first_main,
        [block, block, block]
        + [in_vmem(s) for s in [(64, 512), (64, 512), (16, 8, 512), (16, 8, 512), (8, LANES)]],
        [right_side, reaction, velocity],
        "vvv",
        "v" * 8,
        flops=COST,
    )
    s = right_side
    for iteration in range(ITERS):
        if iteration > 0:
            if iteration + 1 < ITERS:
                r, d, s = call(
                    functools.partial(main, *step_factors(iteration), 1.0 / centre if iteration == 1 else None),
                    [block] * 3,
                    [d, r, s, diag, velocity],
                    "vvvvv",
                    "vvv",
                    flops=COST,
                )
            else:
                r, s = call(last_main, [block, block], [d, r, s, diag, velocity], "vvvvv", "vv", flops=COST)
        if iteration + 1 < ITERS:
            gain = step_factors(iteration)[1]
            scale = 1.0 / centre if iteration == 0 else None
            r, d, *x_faces = call(
                functools.partial(fix_ends, gain, scale),
                [block, block] + face_shapes[:2],
                [*halos, *coefs, r, d],
                "v" * 12,
                "v" * 4,
                aliases={10: 0, 11: 1},
            )
            next_halos = exchange_x(*x_faces)
            r, d, *side_faces = call(
                functools.partial(fix_inner, gain, scale),
                [block, block] + face_shapes[2:],
                [*halos[2:], *coefs[2:], r, d],
                "v" * 8,
                "v" * 5,
                aliases={6: 0, 7: 1},
            )
            halos = next_halos + exchange_sides(*side_faces)
    devices = gx * gy * gz
    residual, part = call(
        last_fix, [block, in_vmem((devices, LANES))], [*halos, *coefs, r], "v" * 11, "vv", aliases={10: 0}
    )
    solution_out = call(
        save, [pltpu.HBM(shape, jnp.float32)], [s], "v", "h", scratch=[pltpu.SemaphoreType.DMA], flops=COST
    )[0]
    part = part.reshape(devices, 1, LANES)
    got = lax.all_to_all(part, ("gx", "gy", "gz"), 0, 0, tiled=True).reshape(devices, LANES)
    cells = shape[0] * shape[1] * shape[2] * devices
    norm = call(functools.partial(finish, cells), [in_vmem((1, LANES))], [got], "v", "v")[0]
    return solution_out, residual, norm[0, 0]


def solution(mesh):
    return jax.shard_map(
        local,
        mesh=mesh,
        in_specs=(P("gx", "gy", "gz"), P("gx", "gy", "gz"), P(None, "gx", "gy", "gz")),
        out_specs=(P("gx", "gy", "gz"), P("gx", "gy", "gz"), P()),
        check_vma=False,
    )
```
